128 devices in a mesh: gx: 8 (over z, y_lo), gy: 8 (over x, core), gz: 2 (over y_hi).
Axes of the slice: x: 4, y: 4 (y_hi: 2, y_lo: 2; y = y_hi * 2 + y_lo), z: 4, core: 2. Of those that a mesh axis runs over, the one named last changes fastest.
Arguments:
- right_side: float32 [512, 512, 512], P('gx', 'gy', 'gz'), may hold values from -6 to 6
- guess: float32 [512, 512, 512], P('gx', 'gy', 'gz'), may hold values from -4 to 4
Outputs:
- updated: float32 [512, 512, 512], P('gx', 'gy', 'gz')
- new_residual: float32 [512, 512, 512], P('gx', 'gy', 'gz')
- res_norm: float32 [], replicated
The draws below stay inside these ranges and needn't reach their ends.
All inputs are finite; a program needn't handle non-finite values.
Results may differ from the reference program's by a relative error of at most 0.0003.
Values sent between devices are 32-bit elements; how exact they have to be, the bound alone decides.
A program may use at most 128 MiB of HBM per device.

```python
import math
import jax
import jax.numpy as jnp

COARSEN = 4
NX = 512
NY = 512
NZ = 512


def level_of(stream_key, shape, pieces, low, top_value):
    loudness = 1.0
    for dim, blocks in pieces:
        heights = jax.random.uniform(jax.random.fold_in(jax.random.fold_in(stream_key, 6), dim), (blocks,), jnp.float32, low / len(pieces), top_value / len(pieces))
        loudness = loudness * jnp.repeat(jnp.exp(heights), shape[dim] // blocks).reshape((-1,) + (1,) * (len(shape) - 1 - dim))
    return loudness


def scatter_about(stream_key, extent, width, reach, pieces=(), kind=jnp.bfloat16):
    array = jax.random.normal(stream_key, extent, jnp.float32) * width
    if len(pieces) > 0:
        array = level_of(stream_key, extent, pieces, -0.22, 0.18) * array
    return jnp.clip(array, min=-reach, max=reach).astype(kind)


def setup_inputs(seed: int = 0) -> dict:
    seeds = jax.random.split(jax.random.key(seed), 3)
    return {
        "right_side": scatter_about(seeds[0], (NX, NY, NZ), 1.0, 6.0, ((0, 8), (1, 8), (2, 2)), jnp.float32),
        "guess": scatter_about(seeds[1], (NX, NY, NZ), 0.5, 4.0, ((0, 8), (1, 8), (2, 2)), jnp.float32),
    }


screen = 0.002

def neighbours(values):
    total = jnp.roll(values, 1, 0) + jnp.roll(values, -1, 0)
    total = total + jnp.roll(values, 1, 1) + jnp.roll(values, -1, 1)
    total = total + jnp.roll(values, 1, 2) + jnp.roll(values, -1, 2)
    return total

def apply_operator(values):
    return (6.0 + screen) * values - neighbours(values)

def eigen_line(length):
    index = jnp.arange(length, dtype=jnp.int32).astype(jnp.float32)
    return (2.0 - 2.0 * jnp.cos(2.0 * math.pi * index / length)) / (COARSEN * COARSEN)

def reference(right_side, guess):
    diag_value = 6.0 + screen
    residual_now = right_side - apply_operator(guess)
    first_sweep = residual_now / diag_value
    local_fix = (residual_now + neighbours(first_sweep)) / diag_value
    coarse_x = NX // COARSEN
    coarse_y = NY // COARSEN
    coarse_z = NZ // COARSEN
    coarse = residual_now.reshape(coarse_x, COARSEN, coarse_y, COARSEN, coarse_z, COARSEN).mean(axis=(1, 3, 5))
    eigen_sum = screen + eigen_line(coarse_x)[:, None, None] + eigen_line(coarse_y)[None, :, None] + eigen_line(coarse_z)[None, None, :]
    spectrum = jnp.fft.fftn(coarse)
    correction = jnp.real(jnp.fft.ifftn(spectrum / eigen_sum)).astype(jnp.float32)
    prolonged = jnp.repeat(jnp.repeat(jnp.repeat(correction, COARSEN, 0), COARSEN, 1), COARSEN, 2)
    updated = guess + local_fix + prolonged
    new_residual = right_side - apply_operator(updated)
    res_norm = jnp.sqrt(jnp.sum(new_residual * new_residual))
    return (updated, new_residual, res_norm)
```

```python
import functools

import jax
import jax.numpy as jnp
import numpy as np
from jax import lax
from jax.experimental import pallas as pl
from jax.experimental.pallas import tpu as pltpu
from jax.sharding import PartitionSpec as P

F32 = jnp.float32
MESH = pl.DeviceIdType.MESH
HIGHEST = lax.Precision.HIGHEST

SCREEN = 0.002
DIAG = 6.0 + SCREEN
INV_DIAG = 1.0 / DIAG

BX, BY, BZ = 64, 64, 256
CX, CY, CZ = 16, 16, 64
NC = 128
GX, GY, GZ = 8, 8, 2
GROUP = GY * GZ
KZ = NC // GROUP
ROWS = 24
CHUNKS = 8
PLANES = BX // CHUNKS


def tables():
    def cas(k, n):
        angle = 2.0 * np.pi * ((k * n) % NC) / NC
        return np.cos(angle) + np.sin(angle)

    mode = np.arange(NC)
    z = np.arange(BZ)
    forward_z = np.zeros((GZ, 2 * BZ, NC))
    inverse_z = np.zeros((GZ, NC, 3 * 128))
    for b in range(GZ):
        cell = CZ * b + z // 4
        here = cas(cell[:, None], mode[None, :])
        before = cas(cell[:, None] - 1, mode[None, :])
        after = cas(cell[:, None] + 1, mode[None, :])
        forward_z[b, :BZ] = here
        forward_z[b, BZ:] = np.where((z % 4 == 0)[:, None], before - here, 0.0) + np.where(
            (z % 4 == 3)[:, None], after - here, 0.0
        )
        inverse_z[b, :, :BZ] = here.T
        inverse_z[b, :, BZ] = cas(CZ * b - 1, mode)
        inverse_z[b, :, 3 * 128 - 1] = cas(CZ * b + CZ, mode)
    forward_y = np.zeros((NC, GY * ROWS))
    for b in range(GY):
        place = np.concatenate([CY * b + np.arange(CY), [CY * b - 1, CY * b + CY]])
        forward_y[:, ROWS * b : ROWS * b + CY + 2] = cas(mode[:, None], place[None, :])
    plain_y = cas(mode[:, None], mode[None, :])
    wave = 2.0 - 2.0 * np.cos(2.0 * np.pi * mode / NC)
    wave_y = np.broadcast_to(wave[:, None], (NC, NC))
    wave_z = np.tile(wave.reshape(GROUP, 1, KZ), (1, CX, 1)).reshape(GROUP, NC)
    out = (forward_z, inverse_z, forward_y, forward_y.T, plain_y, wave_y, wave_z)
    return tuple(np.ascontiguousarray(t, dtype=np.float32) for t in out)


def dot(a, b):
    return jnp.dot(a, b, precision=HIGHEST, preferred_element_type=F32)


def iota(shape, dim):
    return lax.broadcasted_iota(jnp.int32, shape, dim)


def neighbour_sum(a, below, above, row_low, row_high, edge):
    rows, lanes = iota(a.shape, 0), iota(a.shape, 1)
    edges = jnp.concatenate([edge, edge], axis=1)
    total = below + above
    total = total + jnp.where(rows == 0, row_low, pltpu.roll(a, 1, 0))
    total = total + jnp.where(rows == BY - 1, row_high, pltpu.roll(a, BY - 1, 0))
    total = total + jnp.where(lanes == 0, edges, pltpu.roll(a, 1, 1))
    total = total + jnp.where(lanes == BZ - 1, edges, pltpu.roll(a, BZ - 1, 1))
    return total


def pack_edges(a, x, held):
    lane = iota((BY, 128), 1)
    held = jnp.where(lane == x, pltpu.roll(a[:, 128:], x + 1, 1), held)
    return jnp.where(lane == BX + x, pltpu.roll(a[:, :128], BX + x, 1), held)


def unpack_edges(held, x):
    lane = iota((BY, 128), 1)
    low = pltpu.roll(held, lax.rem(128 - x, 128), 1)
    return jnp.where(lane == 0, low, pltpu.roll(held, 63 - x, 1))


def spread_lanes(a):
    a = jnp.where(iota(a.shape, 1) < KZ, a, 0.0)
    for shift in (8, 16, 32, 64):
        a = a + pltpu.roll(a, shift, 1)
    return a


def exchange_kernel(
    rs_hbm, g_hbm, fz_hbm, fy_hbm, iy_hbm, py_hbm, wy_hbm, wz_hbm,
    w_hbm, wx_hbm, wyh_hbm, wzh_hbm, c_hbm,
    g, rs, res, w, fz, fy, iy, py, wy, wz,
    fold, folded, spec, a_send, a_recv, m_send, m_recv, c_send, c_recv,
    y_send, y_recv, z_send, z_recv,
    g_sem, rs_sem, t_sem, out_sem,
    x_ss, x_rs, y_ss, y_rs, z_ss, z_rs, a_ss, a_rs, m_ss, m_rs, c_ss, c_rs, own_sem,
):
    bx, by, bz = lax.axis_index("gx"), lax.axis_index("gy"), lax.axis_index("gz")
    me = bz * GY + by

    barrier = pltpu.get_barrier_semaphore()

    def greet_group(d, _):
        peer = lax.rem(me + d, GROUP)
        pl.semaphore_signal(
            barrier, inc=1, device_id={"gy": lax.rem(peer, GY), "gz": peer // GY}, device_id_type=MESH
        )
        return _

    def greet_line(d, _):
        pl.semaphore_signal(barrier, inc=1, device_id={"gx": lax.rem(bx + d, GX)}, device_id_type=MESH)
        return _

    lax.fori_loop(1, GX, greet_line, 0)
    lax.fori_loop(1, GROUP, greet_group, 0)

    loads_g, loads_rs = [], []
    for c in range(CHUNKS):
        part = pl.ds(PLANES * c, PLANES)
        loads_g.append(
            pltpu.make_async_copy(g_hbm.at[part], g.at[pl.ds(PLANES * c + 1, PLANES)], g_sem.at[c])
        )
        loads_rs.append(pltpu.make_async_copy(rs_hbm.at[part], rs.at[part], rs_sem.at[c]))
    loads_t = [
        pltpu.make_async_copy(src, dst, t_sem.at[i])
        for i, (src, dst) in enumerate(
            ((fz_hbm.at[bz], fz), (fy_hbm, fy), (iy_hbm, iy), (py_hbm, py), (wy_hbm, wy), (wz_hbm, wz))
        )
    ]
    for c in range(CHUNKS):
        loads_g[c].start()
        loads_rs[c].start()
    for load in loads_t:
        load.start()

    pl.semaphore_wait(barrier, GX - 1 + GROUP - 1)

    up_x, down_x = lax.rem(bx + 1, GX), lax.rem(bx + GX - 1, GX)
    up_y, down_y = lax.rem(by + 1, GY), lax.rem(by + GY - 1, GY)

    def planes_out(phase, first, last, array):
        return [
            pltpu.make_async_remote_copy(
                first, array.at[BX + 1], x_ss.at[phase, 0], x_rs.at[phase, 0],
                device_id={"gx": down_x}, device_id_type=MESH,
            ),
            pltpu.make_async_remote_copy(
                last, array.at[0], x_ss.at[phase, 1], x_rs.at[phase, 1],
                device_id={"gx": up_x}, device_id_type=MESH,
            ),
        ]

    def edges_out(phase):
        return [
            pltpu.make_async_remote_copy(
                y_send.at[phase, 0], y_recv.at[phase, 1], y_ss.at[phase, 0], y_rs.at[phase, 0],
                device_id={"gy": down_y}, device_id_type=MESH,
            ),
            pltpu.make_async_remote_copy(
                y_send.at[phase, 1], y_recv.at[phase, 0], y_ss.at[phase, 1], y_rs.at[phase, 1],
                device_id={"gy": up_y}, device_id_type=MESH,
            ),
            pltpu.make_async_remote_copy(
                z_send.at[phase], z_recv.at[phase], z_ss.at[phase], z_rs.at[phase],
                device_id={"gz": 1 - bz}, device_id_type=MESH,
            ),
        ]

    g_planes = planes_out(0, g_hbm.at[0], g_hbm.at[BX - 1], g)
    for copy in g_planes:
        copy.start()

    folded[:, CY:, :] = jnp.zeros((CX, ROWS - CY, 2 * BZ), F32)

    def fold_plane(X, _):
        x = 4 * X + 1
        first, last = g[x], g[x + 3]
        plane = first + g[x + 1] + g[x + 2] + last
        rest = rs[x - 1] + rs[x] + rs[x + 1] + rs[x + 2] - SCREEN * plane
        rest = rest + (g[x - 1] - first) + (g[x + 4] - last)
        rows = iota((CY, 128), 0)
        for half in range(2):
            lanes = slice(128 * half, 128 * (half + 1))
            fold[half] = rest[:, lanes]
            fold[2 + half] = plane[:, lanes]
            a0, a1, a2, a3 = [fold[2 + half, pl.ds(a, CY, stride=4), :] for a in range(4)]
            e0, e1, e2, e3 = [fold[half, pl.ds(a, CY, stride=4), :] for a in range(4)]
            before = jnp.where(rows == 0, 0.0, pltpu.roll(a3, 1, 0))
            after = jnp.where(rows == CY - 1, 0.0, pltpu.roll(a0, CY - 1, 0))
            folded[X, 0:CY, lanes] = (e0 + e1) + (e2 + e3) + (before - a0) + (after - a3)
            folded[X, 0:CY, BZ + 128 * half : BZ + 128 * (half + 1)] = (a0 + a1) + (a2 + a3)
        folded[X, CY : CY + 1, 0:BZ] = plane[0:1, :]
        folded[X, CY + 1 : CY + 2, 0:BZ] = plane[BY - 1 : BY, :]
        return _

    done = 1
    for c in range(CHUNKS):
        loads_g[c].wait()
        loads_rs[c].wait()
        ready = min(CX - 1, (PLANES * (c + 1) - 1) // 4)
        lax.fori_loop(done, ready, fold_plane, 0)
        done = max(done, ready)
    for copy in g_planes:
        copy.wait_recv()
    lax.fori_loop(0, 2, lambda i, _: fold_plane(i * (CX - 1), _), 0)

    for load in loads_t:
        load.wait()

    def modes(X, _):
        spec[X] = pltpu.roll(dot(folded[X], fz[...]), lax.rem(8 * X, 128), 1)
        return _

    lax.fori_loop(0, CX, modes, 0)

    group = iota((ROWS, 128), 1) // KZ

    def copy_a(t, slot):
        return pltpu.make_async_remote_copy(
            a_send.at[t], a_recv.at[slot], a_ss.at[t], a_rs.at[slot],
            device_id={"gy": lax.rem(t, GY), "gz": t // GY}, device_id_type=MESH,
        )

    def send_a(d, _):
        t = lax.rem(me + d, GROUP)
        out = jnp.zeros((ROWS, 128), F32)
        for X in range(CX):
            out = jnp.where(group == lax.rem(t + X, CX), spec[X], out)
        a_send[t] = out
        copy_a(t, me).start()
        return _

    lax.fori_loop(1, GROUP, send_a, 0)
    own = jnp.zeros((ROWS, 128), F32)
    for X in range(CX):
        own = jnp.where(group == lax.rem(me + X, CX), spec[X], own)
    a_recv[me] = own

    lane64 = iota((BY, 128), 1)

    def pack_plane(phase, x, a, held):
        y_send[phase, 0, pl.ds(x, 1), :] = a[0:1, :]
        y_send[phase, 1, pl.ds(x, 1), :] = a[BY - 1 : BY, :]
        return pack_edges(a, x, held)

    z_send[0] = lax.fori_loop(0, BX, lambda x, h: pack_plane(0, x, g[x + 1], h), jnp.zeros((BY, 128), F32))
    g_edges = edges_out(0)
    for copy in g_edges:
        copy.start()

    place = iota((NC, 128), 1) // KZ
    wave = SCREEN * 16.0 + wy[...] + wz[pl.ds(me, 1), :]
    r = 1.0 / (1.0 + 0.5 * wave + jnp.sqrt(wave + 0.25 * wave * wave))
    r2 = r * r
    r4 = r2 * r2
    r8 = r4 * r4
    r16 = r8 * r8

    for copy in g_edges:
        copy.wait_recv()

    def residual_plane(x, held):
        a = g[x + 1]
        total = neighbour_sum(
            a, g[x], g[x + 2], y_recv[0, 0, pl.ds(x, 1), :], y_recv[0, 1, pl.ds(x, 1), :],
            unpack_edges(z_recv[0], x),
        )
        out = rs[x] - (DIAG * a - total)
        res[x + 1] = out
        return pack_plane(1, x, out, held)

    z_send[1] = lax.fori_loop(0, BX, residual_plane, jnp.zeros((BY, 128), F32))
    res_copies = planes_out(1, res.at[1], res.at[BX], res) + edges_out(1)
    for copy in res_copies:
        copy.start()

    def wait_a(d, _):
        t = lax.rem(me + d, GROUP)
        copy_a(t, t).wait_recv()
        return _

    lax.fori_loop(1, GROUP, wait_a, 0)
    lines = (a_recv[0:GY] + a_recv[GY:GROUP]).reshape(GY * ROWS, 128)
    u = pltpu.roll(dot(fy[...], lines), lax.rem(128 - KZ * me + 128, 128), 1)

    right, left = u, u
    for step, power in ((1, r), (2, r2), (4, r4), (8, r8)):
        right = right + jnp.where(place >= step, power * pltpu.roll(right, KZ * step, 1), 0.0)
        left = left + jnp.where(place < CX - step, power * pltpu.roll(left, 128 - KZ * step, 1), 0.0)
    lane = iota((NC, 128), 1)
    ends = jnp.where(lane < KZ, left, pltpu.roll(right, 2 * KZ, 1))
    slot16 = iota((CX, 128), 1) // (2 * KZ)
    packed = jnp.zeros((CX, 128), F32)
    decay = jnp.zeros((CX, 128), F32)
    for i in range(8):
        part = ends[CX * i : CX * (i + 1)]
        packed = jnp.where(slot16 == i, pltpu.roll(part, 2 * KZ * i, 1) if i else part, packed)
        decay = jnp.where(slot16 == i, r16[CX * i : CX * (i + 1)], decay)
    m_send[...] = packed
    m_recv[0] = packed

    def copy_m(d):
        return pltpu.make_async_remote_copy(
            m_send, m_recv.at[d], m_ss.at[d], m_rs.at[d],
            device_id={"gx": lax.rem(bx + d, GX)}, device_id_type=MESH,
        )

    for d in range(1, GX):
        copy_m(d).start()

    end_left, end_right = spread_lanes(left), spread_lanes(pltpu.roll(right, KZ, 1))
    from_low, from_high = r, r
    for bit, power in ((1, r), (2, r2), (4, r4), (8, r8)):
        has = (place // bit) % 2 == 1
        from_low = from_low * jnp.where(has, power, 1.0)
        from_high = from_high * jnp.where(has, 1.0, power)
    scale = (0.25 / (NC * NC)) * r / (1.0 - r2)
    local = right + left - u
    decay8 = decay * decay
    decay8 = decay8 * decay8
    decay8 = decay8 * decay8
    wrap = 1.0 / (1.0 - decay8)

    for copy in res_copies:
        copy.wait_recv()

    def fix_plane(x, held):
        a = res[x + 1]
        total = neighbour_sum(
            a, res[x], res[x + 2], y_recv[1, 0, pl.ds(x, 1), :], y_recv[1, 1, pl.ds(x, 1), :],
            unpack_edges(z_recv[1], x),
        )
        out = g[x + 1] + (a + total * INV_DIAG) * INV_DIAG
        w[x + 1] = out
        return pack_plane(2, x, out, held)

    z_send[2] = lax.fori_loop(0, BX, fix_plane, jnp.zeros((BY, 128), F32))
    w_copies = planes_out(2, w.at[1], w.at[BX], w) + edges_out(2)
    for copy in w_copies:
        copy.start()
    w_out = pltpu.make_async_copy(w.at[pl.ds(1, BX)], w_hbm, out_sem.at[0])
    w_out.start()

    for d in range(1, GX):
        copy_m(d).wait_recv()
    is_right = (iota((CX, 128), 1) // KZ) % 2 == 1
    incoming = jnp.zeros((CX, 128), F32)
    for d in range(GX, 0, -1):
        incoming = jnp.where(is_right, m_recv[d % GX], m_recv[(GX - d) % GX]) + decay * incoming
    incoming = incoming * wrap
    unpacked = jnp.concatenate(
        [pltpu.roll(incoming, 128 - 2 * KZ * i, 1) if i else incoming for i in range(8)], axis=0
    )
    in_left, in_right = spread_lanes(unpacked), spread_lanes(pltpu.roll(unpacked, 128 - KZ, 1))
    solved = scale * (local + from_low * in_right + from_high * in_left)
    before = scale * (r * end_left + in_right + r16 * (r * in_left))
    after = scale * (r * end_right + in_left + r16 * (r * in_right))

    lines = dot(iy[...], pltpu.roll(solved, KZ * me, 1)).reshape(GY, ROWS, 128)
    diagonal = iota((NC, 128), 0) % CY == place
    low = jnp.where(diagonal, dot(py[...], before), 0.0).reshape(GY, CY, 128).sum(axis=1)
    high = jnp.where(diagonal, dot(py[...], after), 0.0).reshape(GY, CY, 128).sum(axis=1)
    c_send[...] = lines
    for b in range(GY):
        c_send[b, CY + 2 : CY + 3, :] = low[b : b + 1]
        c_send[b, CY + 3 : CY + 4, :] = high[b : b + 1]

    def copy_c(t, slot):
        return pltpu.make_async_remote_copy(
            c_send.at[lax.rem(t, GY)], c_recv.at[slot], c_ss.at[t], c_rs.at[slot],
            device_id={"gy": lax.rem(t, GY), "gz": t // GY}, device_id_type=MESH,
        )

    def send_c(d, _):
        copy_c(lax.rem(me + d, GROUP), me).start()
        return _

    lax.fori_loop(1, GROUP, send_c, 0)
    own_copy = pltpu.make_async_copy(c_send.at[by], c_recv.at[me], own_sem)
    own_copy.start()

    for copy in w_copies:
        copy.wait_recv()
    outs = [
        pltpu.make_async_copy(w.at[0], wx_hbm.at[0], out_sem.at[1]),
        pltpu.make_async_copy(w.at[BX + 1], wx_hbm.at[1], out_sem.at[2]),
        pltpu.make_async_copy(y_recv.at[2], wyh_hbm, out_sem.at[3]),
        pltpu.make_async_copy(z_recv.at[2], wzh_hbm, out_sem.at[4]),
    ]
    for copy in outs:
        copy.start()

    own_copy.wait()

    def wait_c(d, _):
        t = lax.rem(me + d, GROUP)
        copy_c(t, t).wait_recv()
        return _

    lax.fori_loop(1, GROUP, wait_c, 0)
    c_out = pltpu.make_async_copy(c_recv, c_hbm, out_sem.at[5])
    c_out.start()

    for copy in g_planes + g_edges + res_copies + w_copies:
        copy.wait_send()

    def wait_sent(d, _):
        t = lax.rem(me + d, GROUP)
        copy_a(t, t).wait_send()
        copy_c(t, t).wait_send()
        return _

    lax.fori_loop(1, GROUP, wait_sent, 0)
    for d in range(1, GX):
        copy_m(d).wait_send()
    w_out.wait()
    for copy in outs:
        copy.wait()
    c_out.wait()


def final_kernel(
    w_hbm, rs_hbm, wx_hbm, wyh_hbm, wzh_hbm, c_hbm, iz_hbm,
    up_hbm, new_hbm, sum_ref,
    up, rs, new, wyh, wzh, c, iz, basis, corr, ends,
    w_sem, rs_sem, s_sem, up_sem, new_sem,
):
    bz = lax.axis_index("gz")
    small = [
        pltpu.make_async_copy(src, dst, s_sem.at[i])
        for i, (src, dst) in enumerate(
            (
                (c_hbm, c), (iz_hbm.at[bz], iz), (wx_hbm.at[0], up.at[0]), (wx_hbm.at[1], up.at[BX + 1]),
                (wyh_hbm, wyh), (wzh_hbm, wzh),
            )
        )
    ]
    loads_w, loads_rs, stores_up, stores_new = [], [], [], []
    for k in range(CHUNKS):
        part, shifted = pl.ds(PLANES * k, PLANES), pl.ds(PLANES * k + 1, PLANES)
        loads_w.append(pltpu.make_async_copy(w_hbm.at[part], up.at[shifted], w_sem.at[k]))
        loads_rs.append(pltpu.make_async_copy(rs_hbm.at[part], rs.at[part], rs_sem.at[k]))
        stores_up.append(pltpu.make_async_copy(up.at[shifted], up_hbm.at[part], up_sem.at[k]))
        stores_new.append(pltpu.make_async_copy(new.at[part], new_hbm.at[part], new_sem.at[k]))
    for copy in small:
        copy.start()
    for k in range(CHUNKS):
        loads_w[k].start()
        loads_rs[k].start()
    for copy in small:
        copy.wait()

    group = iota((ROWS, 128), 1) // KZ

    def gather(X, _):
        out = jnp.zeros((ROWS, 128), F32)
        for t in range(GROUP):
            out = jnp.where(group == lax.rem(X + t, CX), c[t], out)
        basis[X + 1] = pltpu.roll(out, lax.rem(128 - KZ * X + 128, 128), 1)
        return _

    lax.fori_loop(0, CX, gather, 0)
    row, place = iota((CY, 128), 0), iota((CY, 128), 1) // KZ
    for side, X in ((0, 0), (1, CX + 1)):
        out = jnp.zeros((CY, 128), F32)
        for t in range(GROUP):
            line = jnp.where(row == place, c[t, CY + 2 + side : CY + 3 + side, :], 0.0)
            for shift in (8, 16, 32, 64):
                line = line + pltpu.roll(line, shift, 1)
            out = jnp.where(place == t, line, out)
        basis[X, 0:CY, :] = out
        basis[X, CY:, :] = jnp.zeros((ROWS - CY, 128), F32)

    def prolong(X, _):
        out = dot(basis[X], iz[...])
        for part in range(3):
            for a in range(4):
                corr[X, part, pl.ds(a, CY, stride=4), :] = out[0:CY, 128 * part : 128 * (part + 1)]
        ends[X] = out[CY:ROWS]
        return _

    lax.fori_loop(0, CX + 2, prolong, 0)

    def correct(x, X):
        for half in range(2):
            lanes = slice(128 * half, 128 * (half + 1))
            up[x, :, lanes] = up[x, :, lanes] + corr[X, half]

    correct(0, 0)
    correct(BX + 1, CX + 1)

    def update_plane(x, _):
        correct(x + 1, x // 4 + 1)
        return _

    def residual_plane(x, total):
        X = x // 4 + 1
        a = up[x + 1]
        low = wyh[0, pl.ds(x, 1), :] + ends[X, 0:1, 0:BZ]
        high = wyh[1, pl.ds(x, 1), :] + ends[X, 1:2, 0:BZ]
        edge = unpack_edges(wzh[...], x) + corr[X, 2]
        near = neighbour_sum(a, up[x], up[x + 2], low, high, edge)
        out = rs[x] - (DIAG * a - near)
        new[x] = out
        square = out * out
        square = square[:, :128] + square[:, 128:]
        return total + square.reshape(8, 8, 128).sum(axis=0)

    total = jnp.zeros((8, 128), F32)
    done = 0
    for k in range(CHUNKS):
        loads_w[k].wait()
        loads_rs[k].wait()
        lax.fori_loop(PLANES * k, PLANES * (k + 1), update_plane, 0)
        stores_up[k].start()
        ready = BX if k == CHUNKS - 1 else PLANES * (k + 1) - 1
        total = lax.fori_loop(done, ready, residual_plane, total)
        done = ready
        if k > 0:
            stores_new[k - 1].start()
    stores_new[CHUNKS - 1].start()
    sum_ref[...] = total
    for k in range(CHUNKS):
        stores_up[k].wait()
        stores_new[k].wait()


def norm_kernel(part_ref, out_ref, first, second, held, s1, r1, s2, r2):
    bx, by, bz = lax.axis_index("gx"), lax.axis_index("gy"), lax.axis_index("gz")
    planes = GX * GZ
    me = bz * GX + bx
    barrier = pltpu.get_barrier_semaphore()
    for d in range(1, GY):
        pl.semaphore_signal(barrier, inc=1, device_id={"gy": lax.rem(by + d, GY)}, device_id_type=MESH)

    def greet(d, _):
        t = lax.rem(me + d, planes)
        pl.semaphore_signal(
            barrier, inc=1, device_id={"gx": lax.rem(t, GX), "gz": t // GX}, device_id_type=MESH
        )
        return _

    lax.fori_loop(1, planes, greet, 0)
    pl.semaphore_wait(barrier, GY - 1 + planes - 1)

    def copy_1(t, slot):
        return pltpu.make_async_remote_copy(
            part_ref, first.at[slot], s1.at[t], r1.at[slot], device_id={"gy": t}, device_id_type=MESH
        )

    for d in range(1, GY):
        copy_1(lax.rem(by + d, GY), by).start()
    first[by] = part_ref[...]
    for d in range(1, GY):
        t = lax.rem(by + d, GY)
        copy_1(t, t).wait_recv()
    total = first[0]
    for b in range(1, GY):
        total = total + first[b]
    held[...] = total

    def copy_2(t, slot):
        return pltpu.make_async_remote_copy(
            held, second.at[slot], s2.at[t], r2.at[slot],
            device_id={"gx": lax.rem(t, GX), "gz": t // GX}, device_id_type=MESH,
        )

    def send_2(d, _):
        copy_2(lax.rem(me + d, planes), me).start()
        return _

    lax.fori_loop(1, planes, send_2, 0)
    second[me] = total

    def wait_2(d, _):
        t = lax.rem(me + d, planes)
        copy_2(t, t).wait_recv()
        return _

    lax.fori_loop(1, planes, wait_2, 0)
    total = second[0]
    for b in range(1, planes):
        total = total + second[b]
    out_ref[...] = jnp.sqrt(jnp.full((8, 128), jnp.sum(total), F32))

    def wait_sent(d, _):
        t = lax.rem(me + d, planes)
        copy_2(t, t).wait_send()
        return _

    lax.fori_loop(1, planes, wait_sent, 0)
    for d in range(1, GY):
        t = lax.rem(by + d, GY)
        copy_1(t, t).wait_send()


ANY = pl.BlockSpec(memory_space=pl.ANY)
IN_VMEM = pl.BlockSpec(memory_space=pltpu.VMEM)
DMA = pltpu.SemaphoreType.DMA
VMEM = pltpu.VMEM


def per_device(right_side, guess):
    forward_z, inverse_z, forward_y, back_y, plain_y, wave_y, wave_z = [jnp.asarray(t) for t in tables()]
    shape = jax.ShapeDtypeStruct
    block = (BX, BY, BZ)
    padded = (BX + 2, BY, BZ)
    w, wx, wyh, wzh, c = pl.pallas_call(
        exchange_kernel,
        out_shape=(
            shape(block, F32), shape((2, BY, BZ), F32), shape((2, BX, BZ), F32), shape((BY, 128), F32),
            shape((GROUP, ROWS, 128), F32),
        ),
        in_specs=[ANY] * 8,
        out_specs=(ANY,) * 5,
        scratch_shapes=[
            VMEM(padded, F32), VMEM(block, F32), VMEM(padded, F32), VMEM(padded, F32),
            VMEM((2 * BZ, NC), F32), VMEM((NC, GY * ROWS), F32), VMEM((GY * ROWS, NC), F32),
            VMEM((NC, NC), F32), VMEM((NC, NC), F32), VMEM((GROUP, NC), F32),
            VMEM((4, BY, 128), F32), VMEM((CX, ROWS, 2 * BZ), F32), VMEM((CX, ROWS, 128), F32),
            VMEM((GROUP, ROWS, 128), F32), VMEM((GROUP, ROWS, 128), F32),
            VMEM((CX, 128), F32), VMEM((GX, CX, 128), F32),
            VMEM((GY, ROWS, 128), F32), VMEM((GROUP, ROWS, 128), F32),
            VMEM((3, 2, BX, BZ), F32), VMEM((3, 2, BX, BZ), F32), VMEM((3, BY, 128), F32), VMEM((3, BY, 128), F32),
            DMA((CHUNKS,)), DMA((CHUNKS,)), DMA((6,)), DMA((6,)),
            DMA((3, 2)), DMA((3, 2)), DMA((3, 2)), DMA((3, 2)), DMA((3,)), DMA((3,)),
            DMA((GROUP,)), DMA((GROUP,)), DMA((GX,)), DMA((GX,)), DMA((GROUP,)), DMA((GROUP,)), DMA,
        ],
        compiler_params=pltpu.CompilerParams(
            collective_id=0, has_side_effects=True, vmem_limit_bytes=48 * 1024 * 1024
        ),
        name="exchange",
    )(right_side, guess, forward_z, forward_y, back_y, plain_y, wave_y, wave_z)
    updated, new_residual, part = pl.pallas_call(
        final_kernel,
        out_shape=(shape(block, F32), shape(block, F32), shape((8, 128), F32)),
        in_specs=[ANY] * 7,
        out_specs=(ANY, ANY, IN_VMEM),
        scratch_shapes=[
            VMEM(padded, F32), VMEM(block, F32), VMEM(block, F32),
            VMEM((2, BX, BZ), F32), VMEM((BY, 128), F32), VMEM((GROUP, ROWS, 128), F32),
            VMEM((NC, 3 * 128), F32), VMEM((CX + 2, ROWS, 128), F32),
            VMEM((CX + 2, 3, BY, 128), F32), VMEM((CX + 2, ROWS - CY, 3 * 128), F32),
            DMA((CHUNKS,)), DMA((CHUNKS,)), DMA((6,)), DMA((CHUNKS,)), DMA((CHUNKS,)),
        ],
        compiler_params=pltpu.CompilerParams(vmem_limit_bytes=48 * 1024 * 1024),
        name="final",
    )(w, right_side, wx, wyh, wzh, c, inverse_z)
    norm = pl.pallas_call(
        norm_kernel,
        out_shape=shape((8, 128), F32),
        in_specs=[IN_VMEM],
        out_specs=IN_VMEM,
        scratch_shapes=[
            VMEM((GY, 8, 128), F32), VMEM((GX * GZ, 8, 128), F32), VMEM((8, 128), F32),
            DMA((GY,)), DMA((GY,)), DMA((GX * GZ,)), DMA((GX * GZ,)),
        ],
        compiler_params=pltpu.CompilerParams(collective_id=1, has_side_effects=True),
        name="norm",
    )(part)
    return updated, new_residual, norm[0, 0]


def solution(mesh):
    spec = P("gx", "gy", "gz")
    return jax.shard_map(
        per_device, mesh=mesh, in_specs=(spec, spec), out_specs=(spec, spec, P()), check_vma=False
    )
```

```python
import jax
import jax.numpy as jnp
import ml_dtypes
import numpy as np
from jax import lax
from jax.experimental import pallas as pl
from jax.experimental.pallas import tpu as pltpu
from jax.sharding import PartitionSpec as P

F32 = jnp.float32
BF16 = jnp.bfloat16
MESH = pl.DeviceIdType.MESH

SCREEN = 0.002
DIAG = 6.0 + SCREEN
INV_DIAG = 1.0 / DIAG

BX, BY, BZ = 64, 64, 256
CX, CY, CZ = 16, 16, 64
NC = 128
GX, GY, GZ = 8, 8, 2
GROUP = GY * GZ
KZ = NC // GROUP
SENT = 20
ROWS = 24
LOADS = 8
PLANES = BX // LOADS
PARTS = 4
DEEP = BX // PARTS
ORDER = (0, 3, 1, 2)
TOP = 8
PADDED = BY + 16
LOW, MID, HIGH = pl.ds(TOP - 1, BY), pl.ds(TOP, BY), pl.ds(TOP + 1, BY)


def tables():
    def cas(k, n):
        angle = 2.0 * np.pi * ((k * n) % NC) / NC
        return np.cos(angle) + np.sin(angle)

    def pair(t):
        high = t.astype(ml_dtypes.bfloat16)
        low = (t - high.astype(np.float64)).astype(ml_dtypes.bfloat16)
        return np.stack([high, low], axis=-3)

    mode = np.arange(NC)
    z = np.arange(BZ)
    forward_z = np.zeros((GZ, 2 * BZ, NC))
    inverse_z = np.zeros((GZ, NC, 2 * BZ))
    for b in range(GZ):
        cell = CZ * b + z // 4
        here = cas(cell[:, None], mode[None, :])
        down = np.where((z % 4 == 0)[:, None], cas(cell[:, None] - 1, mode[None, :]) - here, 0.0)
        up = np.where((z % 4 == 3)[:, None], cas(cell[:, None] + 1, mode[None, :]) - here, 0.0)
        forward_z[b, :BZ] = here
        forward_z[b, BZ:] = down + up
        inverse_z[b, :, :BZ] = here.T
        inverse_z[b, :, BZ:] = (SCREEN * here - down - up).T
    forward_y = cas(mode[:, None], mode[None, :])
    back_y = np.zeros((GY, ROWS, NC))
    for b in range(GY):
        place = np.concatenate([CY * b + np.arange(CY), [CY * b - 1, CY * b + CY]])
        back_y[b, : CY + 2] = cas(place[:, None], mode[None, :])
    wave = 2.0 - 2.0 * np.cos(2.0 * np.pi * mode / NC)
    wave_y = np.broadcast_to(wave[:, None], (NC, NC)).astype(np.float32)
    wave_z = np.tile(wave.reshape(GROUP, 1, KZ), (1, CX, 1)).reshape(GROUP, NC).astype(np.float32)
    return (
        pair(forward_z), pair(inverse_z), pair(forward_y), pair(back_y.reshape(GY * ROWS, NC)),
        np.ascontiguousarray(wave_y), wave_z,
    )


def split(a):
    high = a.astype(BF16)
    return high, (a - high.astype(F32)).astype(BF16)


def product(a, b):
    return jnp.dot(a, b, preferred_element_type=F32)


def dot_right(a, table):
    high, low = split(a)
    return product(high, table[0]) + (product(high, table[1]) + product(low, table[0]))


def dot_left(table, b):
    high, low = split(b)
    return product(table[0], high) + (product(table[0], low) + product(table[1], high))


def iota(shape, dim):
    return lax.broadcasted_iota(jnp.int32, shape, dim)


def neighbour_sum(ref, p, edges, i):
    lane = iota((BY, 128), 1)
    first, last = lane == 0, lane == 127
    a0, a1 = ref[p, 0, MID, :], ref[p, 1, MID, :]
    low = jnp.concatenate(
        [pltpu.roll(edges, lax.rem(128 - (32 * q + i), 128), 1) for q in range(4)], axis=0
    )
    high = jnp.concatenate([pltpu.roll(edges, 111 - 32 * q - i, 1) for q in range(4)], axis=0)
    up0, up1 = pltpu.roll(a0, 1, 1), pltpu.roll(a1, 1, 1)
    down0, down1 = pltpu.roll(a0, 127, 1), pltpu.roll(a1, 127, 1)
    sums = (
        jnp.where(first, low, up0) + jnp.where(last, down1, down0),
        jnp.where(first, up0, up1) + jnp.where(last, high, down1),
    )
    sums = tuple(
        s + ((ref[p - 1, h, MID, :] + ref[p + 1, h, MID, :]) + (ref[p, h, LOW, :] + ref[p, h, HIGH, :]))
        for h, s in enumerate(sums)
    )
    return (a0, a1), sums


def pack_edges(a0, a1, i, held):
    lane = iota((16, 128), 1)
    for q in range(4):
        rows = slice(16 * q, 16 * (q + 1))
        held = jnp.where(lane == 32 * q + i, pltpu.roll(a1[rows], 32 * q + i + 1, 1), held)
        held = jnp.where(lane == 32 * q + 16 + i, pltpu.roll(a0[rows], 32 * q + 16 + i, 1), held)
    return held


def spread_lanes(a):
    a = jnp.where(iota(a.shape, 1) < KZ, a, 0.0)
    for shift in (8, 16, 32, 64):
        a = a + pltpu.roll(a, shift, 1)
    return a


def kernel(
    rs_hbm, g_hbm, fz_hbm, iz_hbm, fy_hbm, iy_hbm, wy_hbm, wz_hbm,
    up_hbm, new_hbm, norm_ref,
    g, rs, res, w, fz, iz, fy, iy, wy, wz,
    row_y, fold, folded, face_send, face_recv, spec, a_send, a_recv, m_send, m_recv, c_send, c_recv,
    z_send, z_recv, basis, pz, corr, shift, n_send, n_recv, n_held, n_last,
    g_sem, rs_sem, t_sem, row_sem, up_sem, new_sem, own_sem,
    f_ss, f_rs, x_ss, x_rs, y_ss, y_rs, z_ss, z_rs, a_ss, a_rs, m_ss, m_rs, c_ss, c_rs,
    n_ss, n_rs, l_ss, l_rs,
):
    bx, by, bz = lax.axis_index("gx"), lax.axis_index("gy"), lax.axis_index("gz")
    me = bz * GY + by
    up_x, down_x = {"gx": lax.rem(bx + 1, GX)}, {"gx": lax.rem(bx + GX - 1, GX)}
    up_y, down_y = {"gy": lax.rem(by + 1, GY)}, {"gy": lax.rem(by + GY - 1, GY)}

    def of_group(t):
        return {"gy": lax.rem(t, GY), "gz": t // GY}

    def remote(src, dst, send, recv, where):
        return pltpu.make_async_remote_copy(src, dst, send, recv, device_id=where, device_id_type=MESH)

    def others(body):
        def step(d, carry):
            body(lax.rem(me + d, GROUP))
            return carry

        lax.fori_loop(1, GROUP, step, 0)

    barrier = pltpu.get_barrier_semaphore()

    def greet(where):
        pl.semaphore_signal(barrier, inc=1, device_id=where, device_id_type=MESH)

    for d in range(1, GX):
        greet({"gx": lax.rem(bx + d, GX)})
    others(lambda t: greet(of_group(t)))

    halves = [pl.ds(0, 128), pl.ds(128, 128)]
    load_row = [
        pltpu.make_async_copy(g_hbm.at[:, row, halves[h]], row_y.at[side, h], row_sem.at[side, h])
        for side, row in ((0, 0), (1, BY - 1))
        for h in range(2)
    ]
    load_g = [
        [
            pltpu.make_async_copy(
                g_hbm.at[pl.ds(PLANES * c, PLANES), :, halves[h]],
                g.at[pl.ds(PLANES * c + 1, PLANES), h, MID, :],
                g_sem.at[c, h],
            )
            for h in range(2)
        ]
        for c in range(LOADS)
    ]
    load_rs = [
        [
            pltpu.make_async_copy(
                rs_hbm.at[pl.ds(PLANES * c, PLANES), :, halves[h]],
                rs.at[pl.ds(PLANES * c, PLANES), h],
                rs_sem.at[c, h],
            )
            for h in range(2)
        ]
        for c in range(LOADS)
    ]
    load_t = [
        pltpu.make_async_copy(src, dst, t_sem.at[i])
        for i, (src, dst) in enumerate(
            ((fz_hbm.at[bz], fz), (iz_hbm.at[bz], iz), (fy_hbm, fy), (iy_hbm, iy), (wy_hbm, wy), (wz_hbm, wz))
        )
    ]

    def start(copies):
        for copy in copies:
            copy.start()

    def wait(copies):
        for copy in copies:
            copy.wait()

    start(load_g[0])
    start(load_g[LOADS - 1])
    start(load_row)
    start(load_rs[0])
    for c in range(1, LOADS - 1):
        start(load_g[c])
        start(load_rs[c])
    start(load_rs[LOADS - 1])
    start(load_t)

    wait(load_g[0])
    wait(load_g[LOADS - 1])
    wait(load_row)

    def every_fourth(ref, base):
        return [ref[pl.ds(base + a, 16, stride=4), :] for a in range(4)]

    def total_of(four):
        return (four[0] + four[1]) + (four[2] + four[3])

    for h in range(2):
        face_send[0, h] = total_of(every_fourth(g.at[1, h], TOP))
        face_send[1, h] = total_of(every_fourth(g.at[BX, h], TOP))
        face_send[2, h] = total_of(every_fourth(row_y.at[0, h], 0))
        face_send[3, h] = total_of(every_fourth(row_y.at[1, h], 0))
    pl.semaphore_wait(barrier, GX - 1 + GROUP - 1)
    faces = [
        remote(face_send.at[i], face_recv.at[i], f_ss.at[i], f_rs.at[i], where)
        for i, where in enumerate((down_x, up_x, down_y, up_y))
    ]
    start(faces)

    def planes_out(phase, array):
        return {
            0: remote(
                array.at[1, :, MID, :], array.at[BX + 1, :, MID, :],
                x_ss.at[phase, 0], x_rs.at[phase, 0], down_x,
            ),
            PARTS - 1: remote(
                array.at[BX, :, MID, :], array.at[0, :, MID, :], x_ss.at[phase, 1], x_rs.at[phase, 1], up_x
            ),
        }

    def rows_out(phase, array, k):
        part = pl.ds(1 + DEEP * k, DEEP)
        return [
            remote(
                array.at[part, :, pl.ds(TOP, 1), :], array.at[part, :, pl.ds(TOP + BY, 1), :],
                y_ss.at[phase, k, 0], y_rs.at[phase, k, 0], down_y,
            ),
            remote(
                array.at[part, :, pl.ds(TOP + BY - 1, 1), :], array.at[part, :, pl.ds(TOP - 1, 1), :],
                y_ss.at[phase, k, 1], y_rs.at[phase, k, 1], up_y,
            ),
        ]

    def edges_out(phase, k):
        return remote(
            z_send.at[phase, k], z_recv.at[phase, k], z_ss.at[phase, k], z_rs.at[phase, k], {"gz": 1 - bz}
        )

    g_planes = planes_out(0, g)
    start(g_planes.values())

    z_send[0] = jnp.zeros((PARTS, 16, 128), F32)

    def fold_plane(X, has_below=True, has_above=True):
        x = 4 * X + 1
        held = z_send[0, X // 4]
        planes = []
        for j in range(4):
            planes.append((g[x + j, 0, MID, :], g[x + j, 1, MID, :]))
        for h in range(2):
            first, last = planes[0][h], planes[3][h]
            plane = (first + planes[1][h]) + (planes[2][h] + last)
            rest = (rs[x - 1, h] + rs[x, h]) + (rs[x + 1, h] + rs[x + 2, h])
            rest = rest - SCREEN * plane - (first + last)
            if has_below:
                rest = rest + g[x - 1, h, MID, :]
            if has_above:
                rest = rest + g[x + 4, h, MID, :]
            fold[h] = rest
            fold[2 + h] = plane
        rows = iota((CY, 128), 0)
        for h in range(2):
            a = every_fourth(fold.at[2 + h], 0)
            before = jnp.where(rows == 0, 0.0, pltpu.roll(a[3], 1, 0))
            after = jnp.where(rows == CY - 1, 0.0, pltpu.roll(a[0], CY - 1, 0))
            folded[X, :, 128 * h : 128 * (h + 1)] = (
                total_of(every_fourth(fold.at[h], 0)) + (before - a[0]) + (after - a[3])
            )
            folded[X, :, BZ + 128 * h : BZ + 128 * (h + 1)] = total_of(a)
        for j in range(4):
            held = pack_edges(planes[j][0], planes[j][1], 4 * lax.rem(X, 4) + j, held)
        z_send[0, X // 4] = held

    def fold_step(X, carry):
        fold_plane(X)
        return carry

    wait(load_rs[0])
    fold_plane(jnp.int32(0), has_below=False)
    for c in range(1, LOADS - 1):
        wait(load_g[c])
        wait(load_rs[c])
        lax.fori_loop(2 * c - 1, 2 * c + 1, fold_step, 0)
    wait(load_rs[LOADS - 1])
    lax.fori_loop(CX - 3, CX - 1, fold_step, 0)
    fold_plane(jnp.int32(CX - 1), has_above=False)

    for copy in faces:
        copy.wait_recv()
    for h in range(2):
        lanes = slice(128 * h, 128 * (h + 1))
        folded[CX - 1, :, lanes] = folded[CX - 1, :, lanes] + face_recv[0, h]
        folded[0, :, lanes] = folded[0, :, lanes] + face_recv[1, h]
        for X in range(CX):
            folded[X, CY - 1 : CY, lanes] = folded[X, CY - 1 : CY, lanes] + face_recv[2, h, X : X + 1, :]
            folded[X, 0:1, lanes] = folded[X, 0:1, lanes] + face_recv[3, h, X : X + 1, :]

    wait(load_t)
    spec[...] = dot_right(folded[...].reshape(CX * CY, 2 * BZ), fz).reshape(CX, CY, NC)
    for X in range(1, CX):
        spec[X] = pltpu.roll(spec[X], KZ * X, 1)

    group = iota((CY, 128), 1) // KZ

    def message_a(t):
        out = jnp.zeros((CY, 128), F32)
        for X in range(CX):
            out = jnp.where(group == lax.rem(t + X, CX), spec[X], out)
        return out

    def copy_a(t, slot):
        return remote(a_send.at[t], a_recv.at[slot], a_ss.at[t], a_rs.at[slot], of_group(t))

    def send_a(t):
        a_send[t] = message_a(t)
        copy_a(t, me).start()

    others(send_a)
    a_recv[me] = message_a(me)

    g_rows = [copy for k in range(PARTS) for copy in rows_out(0, g, k)]
    g_edges = [edges_out(0, k) for k in range(PARTS)]
    start(g_rows)
    start(g_edges)

    place = iota((NC, 128), 1) // KZ
    wave = SCREEN * 16.0 + wy[...] + wz[pl.ds(me, 1), :]
    r = 1.0 / (1.0 + 0.5 * wave + jnp.sqrt(wave + 0.25 * wave * wave))
    r2 = r * r
    r4 = r2 * r2
    r8 = r4 * r4
    r16 = r8 * r8

    for copy in list(g_planes.values()) + g_rows:
        copy.wait_recv()
    res_planes = planes_out(1, res)
    res_rows = [rows_out(1, res, k) for k in range(PARTS)]
    res_edges = [edges_out(1, k) for k in range(PARTS)]

    def residual_of(k):
        edges = z_recv[0, k]

        def step(i, held):
            x = DEEP * k + i
            a, near = neighbour_sum(g, x + 1, edges, i)
            out = []
            for h in range(2):
                out.append(rs[x, h] - (DIAG * a[h] - near[h]))
                res[x + 1, h, MID, :] = out[h]
            return pack_edges(out[0], out[1], i, held)

        return step

    def by_two(step):
        return lambda i, held: step(2 * i + 1, step(2 * i, held))

    zero = jnp.zeros((16, 128), F32)
    for k in ORDER:
        g_edges[k].wait_recv()
        z_send[1, k] = lax.fori_loop(0, DEEP // 2, by_two(residual_of(k)), zero)
        if k in res_planes:
            res_planes[k].start()
        start(res_rows[k])
        res_edges[k].start()

    others(lambda t: copy_a(t, t).wait_recv())
    lines = (a_recv[0:GY] + a_recv[GY:GROUP]).reshape(NC, 128)
    u = pltpu.roll(dot_left(fy, lines), lax.rem(128 - KZ * me + 128, 128), 1)

    right, left = u, u
    for step, power in ((1, r), (2, r2), (4, r4), (8, r8)):
        right = right + jnp.where(place >= step, power * pltpu.roll(right, KZ * step, 1), 0.0)
        left = left + jnp.where(place < CX - step, power * pltpu.roll(left, 128 - KZ * step, 1), 0.0)
    lane = iota((NC, 128), 1)
    ends = jnp.where(lane < KZ, left, pltpu.roll(right, 2 * KZ, 1))
    slot16 = iota((CX, 128), 1) // (2 * KZ)
    packed = jnp.zeros((CX, 128), F32)
    decay = jnp.zeros((CX, 128), F32)
    for i in range(8):
        part = ends[CX * i : CX * (i + 1)]
        packed = jnp.where(slot16 == i, pltpu.roll(part, 2 * KZ * i, 1) if i else part, packed)
        decay = jnp.where(slot16 == i, r16[CX * i : CX * (i + 1)], decay)
    m_send[...] = packed
    m_recv[0] = packed
    m_copies = [
        remote(m_send, m_recv.at[d], m_ss.at[d], m_rs.at[d], {"gx": lax.rem(bx + d, GX)}) for d in range(1, GX)
    ]
    start(m_copies)

    end_left, end_right = spread_lanes(left), spread_lanes(pltpu.roll(right, KZ, 1))
    from_low, from_high = r, r
    for bit, power in ((1, r), (2, r2), (4, r4), (8, r8)):
        has = (place // bit) % 2 == 1
        from_low = from_low * jnp.where(has, power, 1.0)
        from_high = from_high * jnp.where(has, 1.0, power)
    scale = (0.25 / (NC * NC)) * r / (1.0 - r2)
    local = right + left - u
    decay8 = decay * decay
    decay8 = decay8 * decay8
    decay8 = decay8 * decay8
    wrap = 1.0 / (1.0 - decay8)

    w_planes = planes_out(2, w)
    w_rows = [rows_out(2, w, k) for k in range(PARTS)]
    w_edges = [edges_out(2, k) for k in range(PARTS)]

    def fix_of(k):
        edges = z_recv[1, k]

        def step(i, held):
            x = DEEP * k + i
            a, near = neighbour_sum(res, x + 1, edges, i)
            out = []
            for h in range(2):
                out.append(g[x + 1, h, MID, :] + (a[h] + near[h] * INV_DIAG) * INV_DIAG)
                w[x + 1, h, MID, :] = out[h]
            return pack_edges(out[0], out[1], i, held)

        return step

    for k in ORDER:
        if k in res_planes:
            res_planes[PARTS - 1 - k].wait_recv()
        for copy in res_rows[k] + [res_edges[k]]:
            copy.wait_recv()
        z_send[2, k] = lax.fori_loop(0, DEEP // 2, by_two(fix_of(k)), zero)
        if k in w_planes:
            w_planes[k].start()
        start(w_rows[k])
        w_edges[k].start()

    for copy in m_copies:
        copy.wait_recv()
    is_right = (iota((CX, 128), 1) // KZ) % 2 == 1
    incoming = jnp.zeros((CX, 128), F32)
    for d in range(GX, 0, -1):
        incoming = jnp.where(is_right, m_recv[d % GX], m_recv[(GX - d) % GX]) + decay * incoming
    incoming = incoming * wrap
    unpacked = jnp.concatenate(
        [pltpu.roll(incoming, 128 - 2 * KZ * i, 1) if i else incoming for i in range(8)], axis=0
    )
    in_left, in_right = spread_lanes(unpacked), spread_lanes(pltpu.roll(unpacked, 128 - KZ, 1))
    solved = scale * (local + from_low * in_right + from_high * in_left)
    before = scale * (r * end_left + in_right + r16 * (r * in_left))
    after = scale * (r * end_right + in_left + r16 * (r * in_right))

    lines = dot_left(iy, jnp.concatenate([pltpu.roll(solved, KZ * me, 1), before, after], axis=1))
    diagonal = iota((CY, 128), 0) == iota((CY, 128), 1) // KZ
    for b in range(GY):
        rows = slice(ROWS * b, ROWS * b + CY)
        c_send[b] = lines[ROWS * b : ROWS * (b + 1), :128]
        for side in range(2):
            plane = jnp.where(diagonal, lines[rows, 128 * (side + 1) : 128 * (side + 2)], 0.0)
            c_send[b, CY + 2 + side : CY + 3 + side, :] = jnp.sum(plane, axis=0, keepdims=True)

    sent = pl.ds(0, SENT)

    def copy_c(t, slot):
        return remote(
            c_send.at[lax.rem(t, GY), sent], c_recv.at[slot, sent], c_ss.at[t], c_rs.at[slot], of_group(t)
        )

    others(lambda t: copy_c(t, me).start())
    c_recv[me] = c_send[by]

    def before_of(k):
        edges = z_recv[2, k]

        def step(i, carry):
            x = DEEP * k + i
            a, near = neighbour_sum(w, x + 1, edges, i)
            for h in range(2):
                rs[x, h] = rs[x, h] - (DIAG * a[h] - near[h])
            return carry

        return step

    for k in ORDER:
        if k in w_planes:
            w_planes[PARTS - 1 - k].wait_recv()
        for copy in w_rows[k] + [w_edges[k]]:
            copy.wait_recv()
        lax.fori_loop(0, DEEP // 2, by_two(before_of(k)), 0)

    for copies in (w_rows + [list(w_planes.values())]):
        for copy in copies:
            copy.wait_send()

    others(lambda t: copy_c(t, t).wait_recv())

    group = iota((ROWS, 128), 1) // KZ

    def gather(X):
        out = jnp.zeros((ROWS, 128), F32)
        for t in range(GROUP):
            out = jnp.where(group == lax.rem(X + t, CX), c_recv[t], out)
        basis[X + 1] = pltpu.roll(out, lax.rem(128 - KZ * X + 128, 128), 1)

    def gather_step(i, carry):
        gather(2 * i)
        gather(2 * i + 1)
        return carry

    lax.fori_loop(0, CX // 2, gather_step, 0)
    spot = iota((CY, 128), 1) // KZ
    for side, X in ((0, 0), (1, CX + 1)):
        out = jnp.zeros((CY, 128), F32)
        for t in range(GROUP):
            line = jnp.where(diagonal, c_recv[t, CY + 2 + side : CY + 3 + side, :], 0.0)
            for move in (8, 16, 32, 64):
                line = line + pltpu.roll(line, move, 1)
            out = jnp.where(spot == t, line, out)
        basis[X, 0:CY, :] = out
        basis[X, CY:, :] = jnp.zeros((ROWS - CY, 128), F32)

    pz[...] = dot_right(basis[...].reshape((CX + 2) * ROWS, NC), iz).reshape(CX + 2, ROWS, 2 * BZ)

    def put(ref, X, h, four):
        for a in range(4):
            ref[X, h, pl.ds(a, CY, stride=4), :] = four[a]

    for X in (0, CX + 1):
        for h in range(2):
            put(corr, X, h, [pz[X, 0:CY, 128 * h : 128 * (h + 1)]] * 4)

    def prolong(X, carry):
        row = iota((CY, 128), 0)
        for h in range(2):
            lanes = slice(128 * h, 128 * (h + 1))
            here = pz[X, 0:CY, lanes]
            base = pz[X, 0:CY, BZ + 128 * h : BZ + 128 * (h + 1)]
            below = jnp.where(row == 0, pz[X, CY : CY + 1, lanes], pltpu.roll(here, 1, 0))
            above = jnp.where(row == CY - 1, pz[X, CY + 1 : CY + 2, lanes], pltpu.roll(here, CY - 1, 0))
            put(corr, X, h, [here] * 4)
            put(shift, X - 1, h, [base + (here - below), base, base, base + (here - above)])
        return carry

    lax.fori_loop(1, CX + 1, prolong, 0)

    def finish(X, total):
        for h in range(2):
            here = corr[X + 1, h]
            within = shift[X, h]
            low = here - corr[X, h]
            high = here - corr[X + 2, h]
            for j in range(4):
                x = 4 * X + j
                w[x + 1, h, MID, :] = w[x + 1, h, MID, :] + here
                out = rs[x, h] - within
                if j == 0:
                    out = out - low
                if j == 3:
                    out = out - high
                rs[x, h] = out
                total = total + (out * out).reshape(8, 8, 128).sum(axis=0)
        return total

    total = jnp.zeros((8, 128), F32)
    stores = []
    for c in range(LOADS):
        total = lax.fori_loop(2 * c, 2 * c + 2, finish, total)
        part, shifted = pl.ds(PLANES * c, PLANES), pl.ds(PLANES * c + 1, PLANES)
        now = []
        for h in range(2):
            now.append(
                pltpu.make_async_copy(w.at[shifted, h, MID, :], up_hbm.at[part, :, halves[h]], up_sem.at[c, h])
            )
            now.append(pltpu.make_async_copy(rs.at[part, h], new_hbm.at[part, :, halves[h]], new_sem.at[c, h]))
        start(now)
        stores += now

    n_send[...] = total

    def copy_n(t, slot):
        return remote(n_send, n_recv.at[slot], n_ss.at[t], n_rs.at[slot], of_group(t))

    others(lambda t: copy_n(t, me).start())
    n_recv[me] = total
    others(lambda t: copy_n(t, t).wait_recv())
    total = n_recv[0]
    for t in range(1, GROUP):
        total = total + n_recv[t]
    n_held[...] = total

    def copy_l(d):
        to, slot = lax.rem(bx + d, GX), lax.rem(bx + GX - d, GX)
        return (
            remote(n_held, n_last.at[bx], l_ss.at[d], l_rs.at[bx], {"gx": to}),
            remote(n_held, n_last.at[slot], l_ss.at[d], l_rs.at[slot], {"gx": to}),
        )

    line = [copy_l(d) for d in range(1, GX)]
    for out, _ in line:
        out.start()
    n_last[bx] = total
    for _, back in line:
        back.wait_recv()
    total = n_last[0]
    for b in range(1, GX):
        total = total + n_last[b]
    norm_ref[...] = jnp.sqrt(jnp.full((8, 128), jnp.sum(total), F32))

    for copy in faces + list(g_planes.values()) + g_rows + g_edges + list(res_planes.values()) + res_edges:
        copy.wait_send()
    for copies in res_rows:
        for copy in copies:
            copy.wait_send()
    for copy in w_edges + m_copies:
        copy.wait_send()

    def all_sent(t):
        copy_a(t, t).wait_send()
        copy_c(t, t).wait_send()
        copy_n(t, t).wait_send()

    others(all_sent)
    for out, _ in line:
        out.wait_send()
    wait(stores)


ANY = pl.BlockSpec(memory_space=pl.ANY)
HBM = pl.BlockSpec(memory_space=pltpu.HBM)
IN_VMEM = pl.BlockSpec(memory_space=pltpu.VMEM)
DMA = pltpu.SemaphoreType.DMA
VMEM = pltpu.VMEM


def per_device(right_side, guess):
    shape = jax.ShapeDtypeStruct
    block = (BX, BY, BZ)
    padded = (BX + 2, 2, PADDED, 128)
    updated, new_residual, norm = pl.pallas_call(
        kernel,
        out_shape=(shape(block, F32), shape(block, F32), shape((8, 128), F32)),
        in_specs=[HBM] * 8,
        out_specs=(ANY, ANY, IN_VMEM),
        scratch_shapes=[
            VMEM(padded, F32), VMEM((BX, 2, BY, 128), F32), VMEM(padded, F32), VMEM(padded, F32),
            VMEM((2, 2 * BZ, NC), BF16), VMEM((2, NC, 2 * BZ), BF16), VMEM((2, NC, NC), BF16),
            VMEM((2, GY * ROWS, NC), BF16), VMEM((NC, NC), F32), VMEM((GROUP, NC), F32),
            VMEM((2, 2, BX, 128), F32), VMEM((4, BY, 128), F32), VMEM((CX, CY, 2 * BZ), F32),
            VMEM((4, 2, CX, 128), F32), VMEM((4, 2, CX, 128), F32),
            VMEM((CX, CY, 128), F32), VMEM((GROUP, CY, 128), F32), VMEM((GROUP, CY, 128), F32),
            VMEM((CX, 128), F32), VMEM((GX, CX, 128), F32),
            VMEM((GY, ROWS, 128), F32), VMEM((GROUP, ROWS, 128), F32),
            VMEM((3, PARTS, 16, 128), F32), VMEM((3, PARTS, 16, 128), F32),
            VMEM((CX + 2, ROWS, 128), F32), VMEM((CX + 2, ROWS, 2 * BZ), F32),
            VMEM((CX + 2, 2, BY, 128), F32), VMEM((CX, 2, BY, 128), F32),
            VMEM((8, 128), F32), VMEM((GROUP, 8, 128), F32), VMEM((8, 128), F32), VMEM((GX, 8, 128), F32),
            DMA((LOADS, 2)), DMA((LOADS, 2)), DMA((6,)), DMA((2, 2)), DMA((LOADS, 2)), DMA((LOADS, 2)), DMA,
            DMA((4,)), DMA((4,)), DMA((3, 2)), DMA((3, 2)), DMA((3, PARTS, 2)), DMA((3, PARTS, 2)),
            DMA((3, PARTS)), DMA((3, PARTS)), DMA((GROUP,)), DMA((GROUP,)), DMA((GX,)), DMA((GX,)),
            DMA((GROUP,)), DMA((GROUP,)), DMA((GROUP,)), DMA((GROUP,)), DMA((GX,)), DMA((GX,)),
        ],
        compiler_params=pltpu.CompilerParams(
            collective_id=0, has_side_effects=True, vmem_limit_bytes=48 * 1024 * 1024
        ),
        name="schwarz",
    )(right_side, guess, *[jnp.asarray(t) for t in tables()])
    return updated, new_residual, norm[0, 0]


def solution(mesh):
    spec = P("gx", "gy", "gz")
    return jax.shard_map(
        per_device, mesh=mesh, in_specs=(spec, spec), out_specs=(spec, spec, P()), check_vma=False
    )
```

```python
import math

import jax
import jax.numpy as jnp
from jax import lax
from jax.experimental import pallas as pl
from jax.experimental.pallas import tpu as pltpu
from jax.sharding import PartitionSpec as P

F32 = jnp.float32
BF16 = jnp.bfloat16
MESH = pl.DeviceIdType.MESH

SCREEN = 0.002
DIAG = 6.0 + SCREEN
INV_DIAG = 1.0 / DIAG

BX, BY, BZ = 64, 64, 256
CX, CY, CZ = 16, 16, 64
NC = 128
GX, GY, GZ = 8, 8, 2
GROUP = GY * GZ
KZ = NC // GROUP
ROWS = 24
LOADS = 8
PLANES = BX // LOADS
PARTS = 4
DEEP = BX // PARTS
TOGETHER = 4
ORDER = (0, 3, 1, 2)
TOP = 8
PADDED = BY + 16
LOW, MID, HIGH = pl.ds(TOP - 1, BY), pl.ds(TOP, BY), pl.ds(TOP + 1, BY)


def sine(t):
    a = t.astype(F32) * (math.pi / 128.0)
    b = a * a
    p = -1.0 / 39916800.0
    for c in (1.0 / 362880.0, -1.0 / 5040.0, 1.0 / 120.0, -1.0 / 6.0, 1.0):
        p = p * b + c
    return a * p


def cas(product_of_indices):
    half = sine(jnp.abs(((product_of_indices - 16) & (NC - 1)) - 64))
    return math.sqrt(2.0) * (2.0 * half * half - 1.0)


def wave_of(k):
    half = sine(64 - jnp.abs(k - 64))
    return 4.0 * half * half


def split(a):
    high = a.astype(BF16)
    return high, (a - high.astype(F32)).astype(BF16)


def product(a, b):
    return jnp.dot(a, b, preferred_element_type=F32)


def dot_right(a, table):
    high, low = split(a)
    return product(high, table[0]) + (product(high, table[1]) + product(low, table[0]))


def dot_left(table, b):
    high, low = split(b)
    return product(table[0], high) + (product(table[0], low) + product(table[1], high))


def iota(shape, dim):
    return lax.broadcasted_iota(jnp.int32, shape, dim)


def mod(a, b):
    return a % b if isinstance(a, int) else lax.rem(a, b)


def neighbour_sum(ref, p, edges, i):
    lane = iota((BY, 128), 1)
    first, last = lane == 0, lane == 127
    a0, a1 = ref[p, 0, MID, :], ref[p, 1, MID, :]
    edge = jnp.concatenate([pltpu.roll(edges, 127 - 32 * q - 2 * i, 1) for q in range(4)], axis=0)
    up0, up1 = pltpu.roll(a0, 1, 1), pltpu.roll(a1, 1, 1)
    down0, down1 = pltpu.roll(a0, 127, 1), pltpu.roll(a1, 127, 1)
    sums = (
        jnp.where(first, edge, up0) + jnp.where(last, down1, down0),
        jnp.where(first, up0, up1) + jnp.where(last, edge, down1),
    )
    sums = tuple(
        s + ((ref[p - 1, h, MID, :] + ref[p + 1, h, MID, :]) + (ref[p, h, LOW, :] + ref[p, h, HIGH, :]))
        for h, s in enumerate(sums)
    )
    return (a0, a1), sums


def pack_edges(planes, i, held):
    lane = iota((16, 128), 1)
    end = lane == 127
    for j in range(len(planes) + 1):
        for q in range(4):
            rows = slice(16 * q, 16 * (q + 1))
            place = 32 * q + 2 * (i + j)
            if j == 0:
                value, mask = planes[0][0][rows], lane == place
            elif j == len(planes):
                value, mask = planes[-1][1][rows], lane == place - 1
            else:
                value = jnp.where(end, planes[j - 1][1][rows], planes[j][0][rows])
                mask = (lane == place) | (lane == place - 1)
            held = jnp.where(mask, pltpu.roll(value, mod(place, 128), 1), held)
    return held


def spread_lanes(a):
    a = jnp.where(iota(a.shape, 1) < KZ, a, 0.0)
    for shift in (8, 16, 32, 64):
        a = a + pltpu.roll(a, shift, 1)
    return a


def kernel(
    rs_hbm, g_hbm,
    up_ref, new_ref, norm_ref,
    g, rs, res, w, fz, iz, fy, iy, py,
    fold, folded, extra, spec, a_send, a_recv, m_send, m_recv, v_send, v_recv, c_send, c_recv,
    z_send, z_recv, basis, pz, corr, shift, n_send, n_recv, n_held, n_last,
    g_sem, rs_sem, v_ss, v_rs, x_ss, x_rs, y_ss, y_rs, z_ss, z_rs, a_ss, a_rs, m_ss, m_rs, c_ss, c_rs,
    n_ss, n_rs, l_ss, l_rs,
):
    bx, by, bz = lax.axis_index("gx"), lax.axis_index("gy"), lax.axis_index("gz")
    me = bz * GY + by
    up_x, down_x = {"gx": lax.rem(bx + 1, GX)}, {"gx": lax.rem(bx + GX - 1, GX)}
    up_y, down_y = {"gy": lax.rem(by + 1, GY)}, {"gy": lax.rem(by + GY - 1, GY)}

    def of_group(t):
        return {"gy": lax.rem(t, GY), "gz": t // GY}

    def remote(src, dst, send, recv, where):
        return pltpu.make_async_remote_copy(src, dst, send, recv, device_id=where, device_id_type=MESH)

    def others(body):
        def step(d, carry):
            body(lax.rem(me + d, GROUP))
            return carry

        lax.fori_loop(1, GROUP, step, 0)

    barrier = pltpu.get_barrier_semaphore()

    def greet(where):
        pl.semaphore_signal(barrier, inc=1, device_id=where, device_id_type=MESH)

    for d in range(1, GX):
        greet({"gx": lax.rem(bx + d, GX)})
    others(lambda t: greet(of_group(t)))

    halves = [pl.ds(0, 128), pl.ds(128, 128)]
    load_g = [
        [
            pltpu.make_async_copy(
                g_hbm.at[pl.ds(PLANES * c, PLANES), :, halves[h]],
                g.at[pl.ds(PLANES * c + 1, PLANES), h, MID, :],
                g_sem.at[c, h],
            )
            for h in range(2)
        ]
        for c in range(LOADS)
    ]
    load_rs = [
        [
            pltpu.make_async_copy(
                rs_hbm.at[pl.ds(PLANES * c, PLANES), :, halves[h]],
                rs.at[pl.ds(PLANES * c, PLANES), h],
                rs_sem.at[c, h],
            )
            for h in range(2)
        ]
        for c in range(LOADS)
    ]
    def start(copies):
        for copy in copies:
            copy.start()

    def wait(copies):
        for copy in copies:
            copy.wait()

    start(load_g[0])
    start(load_g[LOADS - 1])
    start(load_rs[0])
    for c in range(1, LOADS - 1):
        start(load_g[c])
        start(load_rs[c])
    start(load_rs[LOADS - 1])

    def keep(ref, rows, lanes, value):
        high, low = split(value)
        ref[0, rows, lanes] = high
        ref[1, rows, lanes] = low

    def beside(z):
        cell = CZ * bz + z // 4
        return cell, cell + jnp.where(z % 4 == 3, 1, 0) - jnp.where(z % 4 == 0, 1, 0)

    whole = slice(None)
    for part in range(4):
        cell, near = beside(iota((64, NC), 0) + 64 * part)
        mode = iota((64, NC), 1)
        here = cas(cell * mode)
        keep(fz, slice(64 * part, 64 * (part + 1)), whole, here)
        keep(fz, slice(BZ + 64 * part, BZ + 64 * (part + 1)), whole, cas(near * mode) - here)
    for part in range(2):
        cell, near = beside(iota((NC, 128), 1) + 128 * part)
        mode = iota((NC, 128), 0)
        here = cas(cell * mode)
        keep(iz, whole, slice(128 * part, 128 * (part + 1)), here)
        keep(iz, whole, slice(BZ + 128 * part, BZ + 128 * (part + 1)), SCREEN * here - (cas(near * mode) - here))

    keep(py, whole, whole, cas(iota((NC, NC), 0) * iota((NC, NC), 1)))

    def place_of(index):
        b = (index * 2731) >> 16
        Y = index - ROWS * b
        place = CY * b + jnp.where(Y == CY, -1, jnp.where(Y == CY + 1, CY, Y))
        return place, Y < CY + 2

    place, used = place_of(iota((NC, GY * ROWS), 1))
    keep(fy, whole, whole, jnp.where(used, cas(place * iota((NC, GY * ROWS), 0)), 0.0))
    place, used = place_of(iota((GY * ROWS, NC), 0))
    keep(iy, whole, whole, jnp.where(used, cas(place * iota((GY * ROWS, NC), 1)), 0.0))

    wait(load_g[0])
    wait(load_g[LOADS - 1])

    def every_fourth(ref, base):
        return [ref[pl.ds(base + a, 16, stride=4), :] for a in range(4)]

    def total_of(four):
        return (four[0] + four[1]) + (four[2] + four[3])

    for h in range(2):
        extra[h, 2 * CX : 3 * CX, :] = total_of(every_fourth(g.at[1, h], TOP))
        extra[h, 3 * CX :, :] = total_of(every_fourth(g.at[BX, h], TOP))

    def planes_out(phase, array):
        return {
            0: remote(
                array.at[1, :, MID, :], array.at[BX + 1, :, MID, :],
                x_ss.at[phase, 0], x_rs.at[phase, 0], down_x,
            ),
            PARTS - 1: remote(
                array.at[BX, :, MID, :], array.at[0, :, MID, :], x_ss.at[phase, 1], x_rs.at[phase, 1], up_x
            ),
        }

    def rows_out(phase, array, k):
        part = pl.ds(1 + DEEP * k, DEEP)
        return [
            remote(
                array.at[part, :, pl.ds(TOP, 1), :], array.at[part, :, pl.ds(TOP + BY, 1), :],
                y_ss.at[phase, k, 0], y_rs.at[phase, k, 0], down_y,
            ),
            remote(
                array.at[part, :, pl.ds(TOP + BY - 1, 1), :], array.at[part, :, pl.ds(TOP - 1, 1), :],
                y_ss.at[phase, k, 1], y_rs.at[phase, k, 1], up_y,
            ),
        ]

    def edges_out(phase, k):
        return remote(
            z_send.at[phase, k], z_recv.at[phase, k], z_ss.at[phase, k], z_rs.at[phase, k], {"gz": 1 - bz}
        )

    z_send[0] = jnp.zeros((PARTS, 16, 128), F32)

    def fold_plane(X, has_below=True, has_above=True):
        x = 4 * X + 1
        planes = []
        for j in range(4):
            planes.append((g[x + j, 0, MID, :], g[x + j, 1, MID, :]))
        for h in range(2):
            first, last = planes[0][h], planes[3][h]
            plane = (first + planes[1][h]) + (planes[2][h] + last)
            rest = (rs[x - 1, h] + rs[x, h]) + (rs[x + 1, h] + rs[x + 2, h])
            rest = rest - SCREEN * plane - (first + last)
            if has_below:
                rest = rest + g[x - 1, h, MID, :]
            if has_above:
                rest = rest + g[x + 4, h, MID, :]
            fold[h] = rest
            fold[2 + h] = plane
        rows = iota((CY, 128), 0)
        for h in range(2):
            a = every_fourth(fold.at[2 + h], 0)
            before = jnp.where(rows == 0, 0.0, pltpu.roll(a[3], 1, 0))
            after = jnp.where(rows == CY - 1, 0.0, pltpu.roll(a[0], CY - 1, 0))
            folded[X, :, 128 * h : 128 * (h + 1)] = (
                total_of(every_fourth(fold.at[h], 0)) + (before - a[0]) + (after - a[3])
            )
            folded[X, :, BZ + 128 * h : BZ + 128 * (h + 1)] = total_of(a)
            extra[h, pl.ds(X, 1), :] = fold[2 + h, 0:1, :]
            extra[h, pl.ds(CX + X, 1), :] = fold[2 + h, BY - 1 : BY, :]
        z_send[0, X // 4] = pack_edges(planes, 4 * mod(X, 4), z_send[0, X // 4])

    def fold_step(X, carry):
        fold_plane(X)
        return carry

    g_planes = planes_out(0, g)
    g_rows = [rows_out(0, g, k) for k in range(PARTS)]
    g_edges = [edges_out(0, k) for k in range(PARTS)]

    def send_part(k):
        start(g_rows[k])
        g_edges[k].start()

    wait(load_rs[0])
    fold_plane(0, has_below=False)
    for c in range(1, LOADS - 1):
        wait(load_g[c])
        wait(load_rs[c])
        lax.fori_loop(2 * c - 1, 2 * c + 1, fold_step, 0)
        if c == 4:
            pl.semaphore_wait(barrier, GX - 1 + GROUP - 1)
            start(g_planes.values())
            send_part(0)
            send_part(1)
    send_part(2)
    wait(load_rs[LOADS - 1])
    lax.fori_loop(CX - 3, CX - 1, fold_step, 0)
    fold_plane(CX - 1, has_above=False)
    send_part(3)

    spec[:, 0:CY, :] = dot_right(folded[...].reshape(CX * CY, 2 * BZ), fz).reshape(CX, CY, NC)
    more = dot_right(jnp.concatenate([extra[0], extra[1]], axis=1), fz.at[:, 0:BZ])
    for X in range(CX):
        spec[X, CY : CY + 1, :] = more[X : X + 1]
        spec[X, CY + 1 : CY + 2, :] = more[CX + X : CX + X + 1]
        if X:
            spec[X, 0 : CY + 2, :] = pltpu.roll(spec[X], KZ * X, 1)[0 : CY + 2]
    row = iota((CY, 128), 0)
    group = iota((CY, 128), 1) // KZ
    sides = []
    for side in range(2):
        plane = more[(2 + side) * CX : (3 + side) * CX]
        for bit in (1, 2, 4, 8):
            plane = jnp.where((row // bit) % 2 == 1, pltpu.roll(plane, KZ * bit, 1), plane)
        sides.append(plane)

    wide = iota((ROWS, 128), 1) // KZ

    def message_a(t, ref, slot):
        out = jnp.zeros((ROWS, 128), F32)
        for X in range(CX):
            out = jnp.where(wide == lax.rem(t + X, CX), spec[X], out)
        ref[slot] = out
        turn = (row + t) % CX
        for side in range(2):
            line = jnp.sum(jnp.where(group == turn, sides[side], 0.0), axis=0, keepdims=True)
            ref[slot, CY + 2 + side : CY + 3 + side, :] = line

    def copy_a(t, slot):
        return remote(a_send.at[t], a_recv.at[slot], a_ss.at[t], a_rs.at[slot], of_group(t))

    def send_a(t):
        message_a(t, a_send, t)
        copy_a(t, me).start()

    others(send_a)
    message_a(me, a_recv, me)

    place = iota((NC, 128), 1) // KZ
    wave = SCREEN * 16.0 + wave_of(iota((NC, 128), 0)) + wave_of(KZ * me + iota((NC, 128), 1) % KZ)
    r = 1.0 / (1.0 + 0.5 * wave + jnp.sqrt(wave + 0.25 * wave * wave))
    r2 = r * r
    r4 = r2 * r2
    r8 = r4 * r4
    r16 = r8 * r8
    inverse = 1.0 / r
    from_low, from_high = r, r
    for bit, power in ((1, r), (2, r2), (4, r4), (8, r8)):
        has = (place // bit) % 2 == 1
        from_low = from_low * jnp.where(has, power, 1.0)
        from_high = from_high * jnp.where(has, 1.0, power)

    for copy in g_planes.values():
        copy.wait_recv()
    res_planes = planes_out(1, res)
    res_rows = [rows_out(1, res, k) for k in range(PARTS)]
    res_edges = [edges_out(1, k) for k in range(PARTS)]

    def residual_of(k):
        edges = z_recv[0, k]

        def step(n, held):
            planes = []
            for j in range(TOGETHER):
                i = TOGETHER * n + j
                x = DEEP * k + i
                a, near = neighbour_sum(g, x + 1, edges, i)
                planes.append([rs[x, h] - (DIAG * a[h] - near[h]) for h in range(2)])
                for h in range(2):
                    res[x + 1, h, MID, :] = planes[j][h]
            return pack_edges(planes, TOGETHER * n, held)

        return step

    zero = jnp.zeros((16, 128), F32)
    for k in ORDER:
        for copy in g_rows[k] + [g_edges[k]]:
            copy.wait_recv()
        z_send[1, k] = lax.fori_loop(0, DEEP // TOGETHER, residual_of(k), zero)
        if k in res_planes:
            res_planes[k].start()
        start(res_rows[k])
        res_edges[k].start()

    others(lambda t: copy_a(t, t).wait_recv())
    lines = a_recv[0:GY] + a_recv[GY:GROUP]
    turn = (row + me) % CX
    beyond = [
        jnp.concatenate(
            [jnp.where(group == turn, lines[b, CY + 2 + side : CY + 3 + side], 0.0) for b in range(GY)], axis=0
        )
        for side in range(2)
    ]
    clean = jnp.where(iota((GY, ROWS, 128), 1) < CY + 2, lines, 0.0).reshape(GY * ROWS, 128)
    u = pltpu.roll(dot_left(fy, clean), lax.rem(128 - KZ * me + 128, 128), 1)
    beyond = dot_left(py, jnp.concatenate(beyond, axis=1))
    out_low, out_high = beyond[:, :128], beyond[:, 128:]
    for move in (8, 16, 32, 64):
        out_low = out_low + pltpu.roll(out_low, move, 1)
        out_high = out_high + pltpu.roll(out_high, move, 1)

    right, left = u, u
    for step, power in ((1, r), (2, r2), (4, r4), (8, r8)):
        right = right + jnp.where(place >= step, power * pltpu.roll(right, KZ * step, 1), 0.0)
        left = left + jnp.where(place < CX - step, power * pltpu.roll(left, 128 - KZ * step, 1), 0.0)
    right = right + from_low * out_low
    left = left + from_high * out_high
    lane = iota((NC, 128), 1)
    outside = jnp.where(lane < KZ, out_low, out_high)
    ends = jnp.where(lane < KZ, left, pltpu.roll(right, 2 * KZ, 1)) + inverse * outside
    slot16 = iota((CX, 128), 1) // (2 * KZ)
    packed = jnp.zeros((CX, 128), F32)
    decay = jnp.zeros((CX, 128), F32)
    packed_out = jnp.zeros((CX, 128), F32)
    for i in range(8):
        part = ends[CX * i : CX * (i + 1)]
        packed = jnp.where(slot16 == i, pltpu.roll(part, 2 * KZ * i, 1) if i else part, packed)
        decay = jnp.where(slot16 == i, r16[CX * i : CX * (i + 1)], decay)
        part = outside[CX * i : CX * (i + 1)]
        packed_out = jnp.where(slot16 == i, pltpu.roll(part, 2 * KZ * i, 1) if i else part, packed_out)
    v_send[...] = packed_out
    m_send[...] = packed
    m_recv[0] = packed
    m_copies = [
        remote(m_send, m_recv.at[d], m_ss.at[d], m_rs.at[d], {"gx": lax.rem(bx + d, GX)}) for d in range(1, GX)
    ]
    start(m_copies)
    v_copies = [
        remote(v_send, v_recv.at[i], v_ss.at[i], v_rs.at[i], where) for i, where in enumerate((up_x, down_x))
    ]
    start(v_copies)

    end_left, end_right = spread_lanes(left), spread_lanes(pltpu.roll(right, KZ, 1))
    scale = (0.25 / (NC * NC)) * r / (1.0 - r2)
    local = right + left - u
    decay8 = decay * decay
    decay8 = decay8 * decay8
    decay8 = decay8 * decay8
    wrap = 1.0 / (1.0 - decay8)

    w_planes = planes_out(2, w)
    w_rows = [rows_out(2, w, k) for k in range(PARTS)]
    w_edges = [edges_out(2, k) for k in range(PARTS)]

    def fix_of(k):
        edges = z_recv[1, k]

        def step(n, held):
            planes = []
            for j in range(TOGETHER):
                i = TOGETHER * n + j
                x = DEEP * k + i
                a, near = neighbour_sum(res, x + 1, edges, i)
                planes.append([g[x + 1, h, MID, :] + (a[h] + near[h] * INV_DIAG) * INV_DIAG for h in range(2)])
                for h in range(2):
                    w[x + 1, h, MID, :] = planes[j][h]
            return pack_edges(planes, TOGETHER * n, held)

        return step

    for k in ORDER:
        if k in res_planes:
            res_planes[PARTS - 1 - k].wait_recv()
        for copy in res_rows[k] + [res_edges[k]]:
            copy.wait_recv()
        z_send[2, k] = lax.fori_loop(0, DEEP // TOGETHER, fix_of(k), zero)
        if k in w_planes:
            w_planes[k].start()
        start(w_rows[k])
        w_edges[k].start()

    for copy in m_copies + v_copies:
        copy.wait_recv()
    is_right = (iota((CX, 128), 1) // KZ) % 2 == 1
    incoming = jnp.zeros((CX, 128), F32)
    for d in range(GX, 0, -1):
        incoming = jnp.where(is_right, m_recv[d % GX], m_recv[(GX - d) % GX]) + decay * incoming
    incoming = incoming * wrap

    def unpack(a):
        return jnp.concatenate(
            [pltpu.roll(a, 128 - 2 * KZ * i, 1) if i else a for i in range(8)], axis=0
        )

    unpacked = unpack(incoming)
    in_left, in_right = spread_lanes(unpacked), spread_lanes(pltpu.roll(unpacked, 128 - KZ, 1))
    near_out = unpack(jnp.where(is_right, v_recv[0], v_recv[1]))
    near_high, near_low = spread_lanes(near_out), spread_lanes(pltpu.roll(near_out, 128 - KZ, 1))
    solved = scale * (local + from_low * in_right + from_high * in_left)
    turned = r - inverse
    before = scale * (out_low + r * end_left + in_right + r16 * (r * in_left) + turned * near_low)
    after = scale * (out_high + r * end_right + in_left + r16 * (r * in_right) + turned * near_high)

    lines = dot_left(iy, jnp.concatenate([pltpu.roll(solved, KZ * me, 1), before, after], axis=1))
    diagonal = iota((CY, 128), 0) == iota((CY, 128), 1) // KZ
    for b in range(GY):
        rows = slice(ROWS * b, ROWS * b + CY)
        c_send[b] = lines[ROWS * b : ROWS * (b + 1), :128]
        for side in range(2):
            plane = jnp.where(diagonal, lines[rows, 128 * (side + 1) : 128 * (side + 2)], 0.0)
            c_send[b, CY + 2 + side : CY + 3 + side, :] = jnp.sum(plane, axis=0, keepdims=True)

    def copy_c(t, slot):
        return remote(c_send.at[lax.rem(t, GY)], c_recv.at[slot], c_ss.at[t], c_rs.at[slot], of_group(t))

    others(lambda t: copy_c(t, me).start())
    c_recv[me] = c_send[by]

    def before_of(k):
        edges = z_recv[2, k]

        def step(n, carry):
            for j in range(TOGETHER):
                i = TOGETHER * n + j
                x = DEEP * k + i
                a, near = neighbour_sum(w, x + 1, edges, i)
                for h in range(2):
                    rs[x, h] = rs[x, h] - (DIAG * a[h] - near[h])
            return carry

        return step

    for k in ORDER:
        if k in w_planes:
            w_planes[PARTS - 1 - k].wait_recv()
        for copy in w_rows[k] + [w_edges[k]]:
            copy.wait_recv()
        lax.fori_loop(0, DEEP // TOGETHER, before_of(k), 0)

    others(lambda t: copy_c(t, t).wait_recv())

    group = iota((ROWS, 128), 1) // KZ

    def gather(X):
        out = jnp.zeros((ROWS, 128), F32)
        for t in range(GROUP):
            out = jnp.where(group == lax.rem(X + t, CX), c_recv[t], out)
        basis[X + 1] = pltpu.roll(out, lax.rem(128 - KZ * X + 128, 128), 1)

    def gather_step(i, carry):
        gather(2 * i)
        gather(2 * i + 1)
        return carry

    lax.fori_loop(0, CX // 2, gather_step, 0)
    spot = iota((CY, 128), 1) // KZ
    for side, X in ((0, 0), (1, CX + 1)):
        out = jnp.zeros((CY, 128), F32)
        for t in range(GROUP):
            line = jnp.where(diagonal, c_recv[t, CY + 2 + side : CY + 3 + side, :], 0.0)
            for move in (8, 16, 32, 64):
                line = line + pltpu.roll(line, move, 1)
            out = jnp.where(spot == t, line, out)
        basis[X, 0:CY, :] = out
        basis[X, CY:, :] = jnp.zeros((ROWS - CY, 128), F32)

    pz[...] = dot_right(basis[...].reshape((CX + 2) * ROWS, NC), iz).reshape(CX + 2, ROWS, 2 * BZ)

    def put(ref, X, h, four):
        for a in range(4):
            ref[X, h, pl.ds(a, CY, stride=4), :] = four[a]

    for X in (0, CX + 1):
        for h in range(2):
            put(corr, X, h, [pz[X, 0:CY, 128 * h : 128 * (h + 1)]] * 4)

    def prolong(X, carry):
        row = iota((CY, 128), 0)
        for h in range(2):
            lanes = slice(128 * h, 128 * (h + 1))
            here = pz[X, 0:CY, lanes]
            base = pz[X, 0:CY, BZ + 128 * h : BZ + 128 * (h + 1)]
            below = jnp.where(row == 0, pz[X, CY : CY + 1, lanes], pltpu.roll(here, 1, 0))
            above = jnp.where(row == CY - 1, pz[X, CY + 1 : CY + 2, lanes], pltpu.roll(here, CY - 1, 0))
            put(corr, X, h, [here] * 4)
            put(shift, X - 1, h, [base + (here - below), base, base, base + (here - above)])
        return carry

    lax.fori_loop(1, CX + 1, prolong, 0)

    def finish(X, total):
        for h in range(2):
            here = corr[X + 1, h]
            within = shift[X, h]
            low = here - corr[X, h]
            high = here - corr[X + 2, h]
            for j in range(4):
                x = 4 * X + j
                lanes = slice(128 * h, 128 * (h + 1))
                up_ref[x, :, lanes] = w[x + 1, h, MID, :] + here
                out = rs[x, h] - within
                if j == 0:
                    out = out - low
                if j == 3:
                    out = out - high
                new_ref[x, :, lanes] = out
                total = total + (out * out).reshape(8, 8, 128).sum(axis=0)
        return total

    total = lax.fori_loop(0, CX, finish, jnp.zeros((8, 128), F32))

    n_send[...] = total

    def copy_n(t, slot):
        return remote(n_send, n_recv.at[slot], n_ss.at[t], n_rs.at[slot], of_group(t))

    others(lambda t: copy_n(t, me).start())
    n_recv[me] = total
    others(lambda t: copy_n(t, t).wait_recv())
    total = n_recv[0]
    for t in range(1, GROUP):
        total = total + n_recv[t]
    n_held[...] = total

    def copy_l(d):
        to, slot = lax.rem(bx + d, GX), lax.rem(bx + GX - d, GX)
        return (
            remote(n_held, n_last.at[bx], l_ss.at[d], l_rs.at[bx], {"gx": to}),
            remote(n_held, n_last.at[slot], l_ss.at[d], l_rs.at[slot], {"gx": to}),
        )

    line = [copy_l(d) for d in range(1, GX)]
    for out, _ in line:
        out.start()
    n_last[bx] = total
    for _, back in line:
        back.wait_recv()
    total = n_last[0]
    for b in range(1, GX):
        total = total + n_last[b]
    norm_ref[...] = jnp.sqrt(jnp.full((8, 128), jnp.sum(total), F32))

    for copy in list(g_planes.values()) + list(res_planes.values()) + list(w_planes.values()):
        copy.wait_send()
    for copies in g_rows + res_rows + w_rows + [g_edges, res_edges, w_edges, m_copies, v_copies]:
        for copy in copies:
            copy.wait_send()

    def all_sent(t):
        copy_a(t, t).wait_send()
        copy_c(t, t).wait_send()
        copy_n(t, t).wait_send()

    others(all_sent)
    for out, _ in line:
        out.wait_send()


ANY = pl.BlockSpec(memory_space=pl.ANY)
IN_VMEM = pl.BlockSpec(memory_space=pltpu.VMEM)
DMA = pltpu.SemaphoreType.DMA
VMEM = pltpu.VMEM


def per_device(right_side, guess):
    shape = jax.ShapeDtypeStruct
    block = (BX, BY, BZ)
    padded = (BX + 2, 2, PADDED, 128)
    updated, new_residual, norm = pl.pallas_call(
        kernel,
        out_shape=(shape(block, F32), shape(block, F32), shape((8, 128), F32)),
        in_specs=[ANY] * 2,
        out_specs=(IN_VMEM,) * 3,
        scratch_shapes=[
            VMEM(padded, F32), VMEM((BX, 2, BY, 128), F32), VMEM(padded, F32), VMEM(padded, F32),
            VMEM((2, 2 * BZ, NC), BF16), VMEM((2, NC, 2 * BZ), BF16), VMEM((2, NC, GY * ROWS), BF16),
            VMEM((2, GY * ROWS, NC), BF16), VMEM((2, NC, NC), BF16),
            VMEM((4, BY, 128), F32), VMEM((CX, CY, 2 * BZ), F32), VMEM((2, 4 * CX, 128), F32),
            VMEM((CX, ROWS, 128), F32), VMEM((GROUP, ROWS, 128), F32), VMEM((GROUP, ROWS, 128), F32),
            VMEM((CX, 128), F32), VMEM((GX, CX, 128), F32), VMEM((CX, 128), F32), VMEM((2, CX, 128), F32),
            VMEM((GY, ROWS, 128), F32), VMEM((GROUP, ROWS, 128), F32),
            VMEM((3, PARTS, 16, 128), F32), VMEM((3, PARTS, 16, 128), F32),
            VMEM((CX + 2, ROWS, 128), F32), VMEM((CX + 2, ROWS, 2 * BZ), F32),
            VMEM((CX + 2, 2, BY, 128), F32), VMEM((CX, 2, BY, 128), F32),
            VMEM((8, 128), F32), VMEM((GROUP, 8, 128), F32), VMEM((8, 128), F32), VMEM((GX, 8, 128), F32),
            DMA((LOADS, 2)), DMA((LOADS, 2)), DMA((2,)), DMA((2,)),
            DMA((3, 2)), DMA((3, 2)), DMA((3, PARTS, 2)), DMA((3, PARTS, 2)),
            DMA((3, PARTS)), DMA((3, PARTS)), DMA((GROUP,)), DMA((GROUP,)), DMA((GX,)), DMA((GX,)),
            DMA((GROUP,)), DMA((GROUP,)), DMA((GROUP,)), DMA((GROUP,)), DMA((GX,)), DMA((GX,)),
        ],
        compiler_params=pltpu.CompilerParams(
            collective_id=0, has_side_effects=True, vmem_limit_bytes=44 * 1024 * 1024
        ),
        name="schwarz",
    )(right_side, guess)
    return updated, new_residual, norm[0, 0]


def solution(mesh):
    spec = P("gx", "gy", "gz")
    return jax.shard_map(
        per_device, mesh=mesh, in_specs=(spec, spec), out_specs=(spec, spec, P()), check_vma=False
    )
```

```python
import math

import jax
import jax.numpy as jnp
from jax import lax
from jax.experimental import pallas as pl
from jax.experimental.pallas import tpu as pltpu
from jax.sharding import PartitionSpec as P

F32 = jnp.float32
BF16 = jnp.bfloat16
MESH = pl.DeviceIdType.MESH

SCREEN = 0.002
DIAG = 6.0 + SCREEN
INV_DIAG = 1.0 / DIAG

BX, BY, BZ = 64, 64, 256
CX, CY, CZ = 16, 16, 64
NC = 128
GX, GY, GZ = 8, 8, 2
GROUP = GY * GZ
KZ = NC // GROUP
EXTRA = 4
ROWS = 24
LOADS = 8
PLANES = BX // LOADS
PARTS = 4
DEEP = BX // PARTS
TOGETHER = 4
ORDER = (0, 3, 1, 2)
TOP = 8
PADDED = BY + 16
LOW, MID, HIGH = pl.ds(TOP - 1, BY), pl.ds(TOP, BY), pl.ds(TOP + 1, BY)


def sine(t):
    a = t.astype(F32) * (math.pi / 128.0)
    b = a * a
    p = -1.0 / 39916800.0
    for c in (1.0 / 362880.0, -1.0 / 5040.0, 1.0 / 120.0, -1.0 / 6.0, 1.0):
        p = p * b + c
    return a * p


def cas(product_of_indices):
    half = sine(jnp.abs(((product_of_indices - 16) & (NC - 1)) - 64))
    return math.sqrt(2.0) * (2.0 * half * half - 1.0)


def wave_of(k):
    half = sine(64 - jnp.abs(k - 64))
    return 4.0 * half * half


def split(a):
    high = a.astype(BF16)
    return high, (a - high.astype(F32)).astype(BF16)


def product(a, b):
    return jnp.dot(a, b, preferred_element_type=F32)


def dot_right(a, table):
    high, low = split(a)
    return product(high, table[0]) + (product(high, table[1]) + product(low, table[0]))


def dot_left(table, b):
    high, low = split(b)
    return product(table[0], high) + (product(table[0], low) + product(table[1], high))


def iota(shape, dim):
    return lax.broadcasted_iota(jnp.int32, shape, dim)


def mod(a, b):
    return a % b if isinstance(a, int) else lax.rem(a, b)


def neighbour_sum(ref, p, edges, i):
    lane = iota((BY, 128), 1)
    first, last = lane == 0, lane == 127
    a0, a1 = ref[p, 0, MID, :], ref[p, 1, MID, :]
    edge = jnp.concatenate([pltpu.roll(edges, 127 - 32 * q - 2 * i, 1) for q in range(4)], axis=0)
    up0, up1 = pltpu.roll(a0, 1, 1), pltpu.roll(a1, 1, 1)
    down0, down1 = pltpu.roll(a0, 127, 1), pltpu.roll(a1, 127, 1)
    sums = (
        jnp.where(first, edge, up0) + jnp.where(last, down1, down0),
        jnp.where(first, up0, up1) + jnp.where(last, edge, down1),
    )
    sums = tuple(
        s + ((ref[p - 1, h, MID, :] + ref[p + 1, h, MID, :]) + (ref[p, h, LOW, :] + ref[p, h, HIGH, :]))
        for h, s in enumerate(sums)
    )
    return (a0, a1), sums


def pack_edges(planes, i, held):
    lane = iota((16, 128), 1)
    end = lane == 127
    for j in range(len(planes) + 1):
        for q in range(4):
            rows = slice(16 * q, 16 * (q + 1))
            place = 32 * q + 2 * (i + j)
            if j == 0:
                value, mask = planes[0][0][rows], lane == place
            elif j == len(planes):
                value, mask = planes[-1][1][rows], lane == place - 1
            else:
                value = jnp.where(end, planes[j - 1][1][rows], planes[j][0][rows])
                mask = (lane == place) | (lane == place - 1)
            held = jnp.where(mask, pltpu.roll(value, mod(place, 128), 1), held)
    return held


def spread_lanes(a):
    a = jnp.where(iota(a.shape, 1) < KZ, a, 0.0)
    for shift in (8, 16, 32, 64):
        a = a + pltpu.roll(a, shift, 1)
    return a


def kernel(
    rs_hbm, g_hbm,
    up_ref, new_ref, norm_ref,
    g, rs, res, w, fz, iz, py, fe, ie,
    fold, folded, extra, spec, a_send, a_recv, ae_send, ae_recv, lines_e, m_send, m_recv, v_send, v_recv, c_send, c_recv, ce_send, ce_recv,
    z_send, z_recv, basis, pz, corr, shift, n_send, n_recv, n_held, n_last,
    g_sem, rs_sem, v_ss, v_rs, x_ss, x_rs, y_ss, y_rs, z_ss, z_rs, a_ss, a_rs, m_ss, m_rs, c_ss, c_rs, ae_ss, ae_rs, ce_ss, ce_rs,
    n_ss, n_rs, l_ss, l_rs,
):
    bx, by, bz = lax.axis_index("gx"), lax.axis_index("gy"), lax.axis_index("gz")
    me = bz * GY + by
    up_x, down_x = {"gx": lax.rem(bx + 1, GX)}, {"gx": lax.rem(bx + GX - 1, GX)}
    up_y, down_y = {"gy": lax.rem(by + 1, GY)}, {"gy": lax.rem(by + GY - 1, GY)}

    def of_group(t):
        return {"gy": lax.rem(t, GY), "gz": t // GY}

    def remote(src, dst, send, recv, where):
        return pltpu.make_async_remote_copy(src, dst, send, recv, device_id=where, device_id_type=MESH)

    def others(body):
        def across(d, carry):
            body((1 - bz) * GY + lax.rem(by + d, GY))
            return carry

        def along(d, carry):
            body(bz * GY + lax.rem(by + d, GY))
            return carry

        lax.fori_loop(0, GY, across, 0)
        lax.fori_loop(1, GY, along, 0)

    barrier = pltpu.get_barrier_semaphore()

    def greet(where):
        pl.semaphore_signal(barrier, inc=1, device_id=where, device_id_type=MESH)

    for d in range(1, GX):
        greet({"gx": lax.rem(bx + d, GX)})
    others(lambda t: greet(of_group(t)))

    halves = [pl.ds(0, 128), pl.ds(128, 128)]
    load_g = [
        [
            pltpu.make_async_copy(
                g_hbm.at[pl.ds(PLANES * c, PLANES), :, halves[h]],
                g.at[pl.ds(PLANES * c + 1, PLANES), h, MID, :],
                g_sem.at[c, h],
            )
            for h in range(2)
        ]
        for c in range(LOADS)
    ]
    load_rs = [
        [
            pltpu.make_async_copy(
                rs_hbm.at[pl.ds(PLANES * c, PLANES), :, halves[h]],
                rs.at[pl.ds(PLANES * c, PLANES), h],
                rs_sem.at[c, h],
            )
            for h in range(2)
        ]
        for c in range(LOADS)
    ]
    def start(copies):
        for copy in copies:
            copy.start()

    def wait(copies):
        for copy in copies:
            copy.wait()

    def wait_recv(copies):
        for copy in copies:
            copy.wait_recv()

    def wait_send(copies):
        for copy in copies:
            copy.wait_send()

    start(load_g[0])
    start(load_g[LOADS - 1])
    start(load_rs[0])
    for c in range(1, LOADS - 1):
        start(load_g[c])
        start(load_rs[c])
    start(load_rs[LOADS - 1])

    def keep(ref, rows, lanes, value):
        high, low = split(value)
        ref[0, rows, lanes] = high
        ref[1, rows, lanes] = low

    def beside(z):
        cell = CZ * bz + z // 4
        return cell, cell + jnp.where(z % 4 == 3, 1, 0) - jnp.where(z % 4 == 0, 1, 0)

    whole = slice(None)
    for part in range(4):
        cell, near = beside(iota((64, NC), 0) + 64 * part)
        mode = iota((64, NC), 1)
        here = cas(cell * mode)
        keep(fz, slice(64 * part, 64 * (part + 1)), whole, here)
        keep(fz, slice(BZ + 64 * part, BZ + 64 * (part + 1)), whole, cas(near * mode) - here)
    for part in range(2):
        cell, near = beside(iota((NC, 128), 1) + 128 * part)
        mode = iota((NC, 128), 0)
        here = cas(cell * mode)
        keep(iz, whole, slice(128 * part, 128 * (part + 1)), here)
        keep(iz, whole, slice(BZ + 128 * part, BZ + 128 * (part + 1)), SCREEN * here - (cas(near * mode) - here))

    keep(py, whole, whole, cas(iota((NC, NC), 0) * iota((NC, NC), 1)))

    def place_of(index):
        e = index % EXTRA
        return CY * (index // EXTRA) + jnp.where(e == 0, -1, CY), e < 2

    place, used = place_of(iota((NC, GY * EXTRA), 1))
    keep(fe, whole, whole, jnp.where(used, cas(place * iota((NC, GY * EXTRA), 0)), 0.0))
    place, used = place_of(iota((GY * EXTRA, NC), 0))
    keep(ie, whole, whole, jnp.where(used, cas(place * iota((GY * EXTRA, NC), 1)), 0.0))

    wait(load_g[0])
    wait(load_g[LOADS - 1])

    def every_fourth(ref, base):
        return [ref[pl.ds(base + a, 16, stride=4), :] for a in range(4)]

    def total_of(four):
        return (four[0] + four[1]) + (four[2] + four[3])

    for h in range(2):
        extra[h, 2 * CX : 3 * CX, :] = total_of(every_fourth(g.at[1, h], TOP))
        extra[h, 3 * CX :, :] = total_of(every_fourth(g.at[BX, h], TOP))

    def planes_out(phase, array):
        return {
            0: remote(
                array.at[1, :, MID, :], array.at[BX + 1, :, MID, :],
                x_ss.at[phase, 0], x_rs.at[phase, 0], down_x,
            ),
            PARTS - 1: remote(
                array.at[BX, :, MID, :], array.at[0, :, MID, :], x_ss.at[phase, 1], x_rs.at[phase, 1], up_x
            ),
        }

    def rows_out(phase, array, k):
        part = pl.ds(1 + DEEP * k, DEEP)
        return [
            remote(
                array.at[part, :, pl.ds(TOP, 1), :], array.at[part, :, pl.ds(TOP + BY, 1), :],
                y_ss.at[phase, k, 0], y_rs.at[phase, k, 0], down_y,
            ),
            remote(
                array.at[part, :, pl.ds(TOP + BY - 1, 1), :], array.at[part, :, pl.ds(TOP - 1, 1), :],
                y_ss.at[phase, k, 1], y_rs.at[phase, k, 1], up_y,
            ),
        ]

    def edges_out(phase, k):
        return remote(
            z_send.at[phase, k], z_recv.at[phase, k], z_ss.at[phase, k], z_rs.at[phase, k], {"gz": 1 - bz}
        )

    z_send[0] = jnp.zeros((PARTS, 16, 128), F32)

    def fold_plane(X, has_below=True, has_above=True):
        x = 4 * X + 1
        planes = []
        for j in range(4):
            planes.append((g[x + j, 0, MID, :], g[x + j, 1, MID, :]))
        for h in range(2):
            first, last = planes[0][h], planes[3][h]
            plane = (first + planes[1][h]) + (planes[2][h] + last)
            rest = (rs[x - 1, h] + rs[x, h]) + (rs[x + 1, h] + rs[x + 2, h])
            rest = rest - SCREEN * plane - (first + last)
            if has_below:
                rest = rest + g[x - 1, h, MID, :]
            if has_above:
                rest = rest + g[x + 4, h, MID, :]
            fold[h] = rest
            fold[2 + h] = plane
        rows = iota((CY, 128), 0)
        for h in range(2):
            a = every_fourth(fold.at[2 + h], 0)
            before = jnp.where(rows == 0, 0.0, pltpu.roll(a[3], 1, 0))
            after = jnp.where(rows == CY - 1, 0.0, pltpu.roll(a[0], CY - 1, 0))
            folded[X, :, 128 * h : 128 * (h + 1)] = (
                total_of(every_fourth(fold.at[h], 0)) + (before - a[0]) + (after - a[3])
            )
            folded[X, :, BZ + 128 * h : BZ + 128 * (h + 1)] = total_of(a)
            extra[h, pl.ds(X, 1), :] = fold[2 + h, 0:1, :]
            extra[h, pl.ds(CX + X, 1), :] = fold[2 + h, BY - 1 : BY, :]
        z_send[0, X // 4] = pack_edges(planes, 4 * mod(X, 4), z_send[0, X // 4])

    def fold_step(X, carry):
        fold_plane(X)
        return carry

    g_planes = planes_out(0, g)
    g_rows = [rows_out(0, g, k) for k in range(PARTS)]
    g_edges = [edges_out(0, k) for k in range(PARTS)]

    wait(load_rs[0])
    fold_plane(0, has_below=False)
    for c in range(1, LOADS - 1):
        wait(load_g[c])
        wait(load_rs[c])
        lax.fori_loop(2 * c - 1, 2 * c + 1, fold_step, 0)
    wait(load_rs[LOADS - 1])
    lax.fori_loop(CX - 3, CX - 1, fold_step, 0)
    fold_plane(CX - 1, has_above=False)

    spec[...] = dot_right(folded[...].reshape(CX * CY, 2 * BZ), fz).reshape(CX, CY, NC)
    more = dot_right(jnp.concatenate([extra[0], extra[1]], axis=1), fz.at[:, 0:BZ])
    for X in range(1, CX):
        spec[X] = pltpu.roll(spec[X], KZ * X, 1)
    row = iota((CY, 128), 0)
    group = iota((CY, 128), 1) // KZ
    sides = []
    for e in range(EXTRA):
        plane = more[CX * e : CX * (e + 1)]
        for bit in (1, 2, 4, 8):
            plane = jnp.where((row // bit) % 2 == 1, pltpu.roll(plane, KZ * bit, 1), plane)
        sides.append(plane)
    pl.semaphore_wait(barrier, GX - 1 + GROUP - 1)

    def message_a(t, ref, ref_e, slot):
        out = jnp.zeros((CY, 128), F32)
        for X in range(CX):
            out = jnp.where(group == lax.rem(t + X, CX), spec[X], out)
        ref[slot] = out
        turn = group == (row + t) % CX
        for e in range(EXTRA):
            ref_e[slot, e : e + 1, :] = jnp.sum(jnp.where(turn, sides[e], 0.0), axis=0, keepdims=True)

    def copy_a(t, slot):
        return (
            remote(a_send.at[t], a_recv.at[slot], a_ss.at[t], a_rs.at[slot], of_group(t)),
            remote(ae_send.at[t], ae_recv.at[slot], ae_ss.at[t], ae_rs.at[slot], of_group(t)),
        )

    def send_a(t):
        message_a(t, a_send, ae_send, t)
        start(copy_a(t, me))

    others(send_a)
    message_a(me, a_recv, ae_recv, me)
    start(g_planes.values())
    for k in ORDER:
        start(g_rows[k])
        g_edges[k].start()

    place = iota((NC, 128), 1) // KZ
    wave = SCREEN * 16.0 + wave_of(iota((NC, 128), 0)) + wave_of(KZ * me + iota((NC, 128), 1) % KZ)
    r = 1.0 / (1.0 + 0.5 * wave + jnp.sqrt(wave + 0.25 * wave * wave))
    r2 = r * r
    r4 = r2 * r2
    r8 = r4 * r4
    r16 = r8 * r8
    inverse = 1.0 / r
    from_low, from_high = r, r
    for bit, power in ((1, r), (2, r2), (4, r4), (8, r8)):
        has = (place // bit) % 2 == 1
        from_low = from_low * jnp.where(has, power, 1.0)
        from_high = from_high * jnp.where(has, 1.0, power)

    others(lambda t: wait_recv(copy_a(t, t)))
    lines = (a_recv[0:GY] + a_recv[GY:GROUP]).reshape(NC, 128)
    turn = group == (row + me) % CX
    beyond = [[], []]
    for b in range(GY):
        four = ae_recv[b] + ae_recv[GY + b]
        lines_e[EXTRA * b : EXTRA * (b + 1), :] = four
        for side in range(2):
            beyond[side].append(jnp.where(turn, four[2 + side : 3 + side], 0.0))
    u = dot_left(py, lines) + dot_left(fe, lines_e[...])
    u = pltpu.roll(u, lax.rem(128 - KZ * me + 128, 128), 1)
    beyond = jnp.concatenate([jnp.concatenate(beyond[side], axis=0) for side in range(2)], axis=1)
    beyond = dot_left(py, beyond)
    out_low, out_high = beyond[:, :128], beyond[:, 128:]
    for move in (8, 16, 32, 64):
        out_low = out_low + pltpu.roll(out_low, move, 1)
        out_high = out_high + pltpu.roll(out_high, move, 1)

    right, left = u, u
    for step, power in ((1, r), (2, r2), (4, r4), (8, r8)):
        right = right + jnp.where(place >= step, power * pltpu.roll(right, KZ * step, 1), 0.0)
        left = left + jnp.where(place < CX - step, power * pltpu.roll(left, 128 - KZ * step, 1), 0.0)
    right = right + from_low * out_low
    left = left + from_high * out_high
    lane = iota((NC, 128), 1)
    outside = jnp.where(lane < KZ, out_low, out_high)
    ends = jnp.where(lane < KZ, left, pltpu.roll(right, 2 * KZ, 1)) + inverse * outside
    slot16 = iota((CX, 128), 1) // (2 * KZ)
    packed = jnp.zeros((CX, 128), F32)
    decay = jnp.zeros((CX, 128), F32)
    packed_out = jnp.zeros((CX, 128), F32)
    for i in range(8):
        part = ends[CX * i : CX * (i + 1)]
        packed = jnp.where(slot16 == i, pltpu.roll(part, 2 * KZ * i, 1) if i else part, packed)
        decay = jnp.where(slot16 == i, r16[CX * i : CX * (i + 1)], decay)
        part = outside[CX * i : CX * (i + 1)]
        packed_out = jnp.where(slot16 == i, pltpu.roll(part, 2 * KZ * i, 1) if i else part, packed_out)
    v_send[...] = packed_out
    m_send[...] = packed
    m_recv[0] = packed
    m_copies = [
        remote(m_send, m_recv.at[d], m_ss.at[d], m_rs.at[d], {"gx": lax.rem(bx + d, GX)}) for d in range(1, GX)
    ]
    start(m_copies)
    v_copies = [
        remote(v_send, v_recv.at[i], v_ss.at[i], v_rs.at[i], where) for i, where in enumerate((up_x, down_x))
    ]
    start(v_copies)

    end_left, end_right = spread_lanes(left), spread_lanes(pltpu.roll(right, KZ, 1))
    scale = (0.25 / (NC * NC)) * r / (1.0 - r2)
    local = right + left - u
    decay8 = decay * decay
    decay8 = decay8 * decay8
    decay8 = decay8 * decay8
    wrap = 1.0 / (1.0 - decay8)

    for copy in g_planes.values():
        copy.wait_recv()
    res_planes = planes_out(1, res)
    res_rows = [rows_out(1, res, k) for k in range(PARTS)]
    res_edges = [edges_out(1, k) for k in range(PARTS)]

    def residual_of(k):
        edges = z_recv[0, k]

        def step(n, held):
            planes = []
            for j in range(TOGETHER):
                i = TOGETHER * n + j
                x = DEEP * k + i
                a, near = neighbour_sum(g, x + 1, edges, i)
                planes.append([rs[x, h] - (DIAG * a[h] - near[h]) for h in range(2)])
                for h in range(2):
                    res[x + 1, h, MID, :] = planes[j][h]
            return pack_edges(planes, TOGETHER * n, held)

        return step

    zero = jnp.zeros((16, 128), F32)
    for k in ORDER:
        for copy in g_rows[k] + [g_edges[k]]:
            copy.wait_recv()
        z_send[1, k] = lax.fori_loop(0, DEEP // TOGETHER, residual_of(k), zero)
        if k in res_planes:
            res_planes[k].start()
        start(res_rows[k])
        res_edges[k].start()

    for copy in m_copies + v_copies:
        copy.wait_recv()
    is_right = (iota((CX, 128), 1) // KZ) % 2 == 1
    incoming = jnp.zeros((CX, 128), F32)
    for d in range(GX, 0, -1):
        incoming = jnp.where(is_right, m_recv[d % GX], m_recv[(GX - d) % GX]) + decay * incoming
    incoming = incoming * wrap

    def unpack(a):
        return jnp.concatenate(
            [pltpu.roll(a, 128 - 2 * KZ * i, 1) if i else a for i in range(8)], axis=0
        )

    unpacked = unpack(incoming)
    in_left, in_right = spread_lanes(unpacked), spread_lanes(pltpu.roll(unpacked, 128 - KZ, 1))
    near_out = unpack(jnp.where(is_right, v_recv[0], v_recv[1]))
    near_high, near_low = spread_lanes(near_out), spread_lanes(pltpu.roll(near_out, 128 - KZ, 1))
    solved = scale * (local + from_low * in_right + from_high * in_left)
    turned = r - inverse
    before = scale * (out_low + r * end_left + in_right + r16 * (r * in_left) + turned * near_low)
    after = scale * (out_high + r * end_right + in_left + r16 * (r * in_right) + turned * near_high)

    back = pltpu.roll(solved, KZ * me, 1)
    lines = dot_left(py, jnp.concatenate([back, before, after], axis=1))
    ends = dot_left(ie, back)
    diagonal = iota((CY, 128), 0) == iota((CY, 128), 1) // KZ
    for b in range(GY):
        rows = slice(CY * b, CY * (b + 1))
        c_send[b] = lines[rows, :128]
        ce_send[b, 0:2, :] = ends[EXTRA * b : EXTRA * b + 2]
        for side in range(2):
            plane = jnp.where(diagonal, lines[rows, 128 * (side + 1) : 128 * (side + 2)], 0.0)
            ce_send[b, 2 + side : 3 + side, :] = jnp.sum(plane, axis=0, keepdims=True)

    def copy_c(t, slot):
        b = lax.rem(t, GY)
        return (
            remote(c_send.at[b], c_recv.at[slot], c_ss.at[t], c_rs.at[slot], of_group(t)),
            remote(ce_send.at[b], ce_recv.at[slot], ce_ss.at[t], ce_rs.at[slot], of_group(t)),
        )

    others(lambda t: start(copy_c(t, me)))
    c_recv[me] = c_send[by]
    ce_recv[me] = ce_send[by]

    w_planes = planes_out(2, w)
    w_rows = [rows_out(2, w, k) for k in range(PARTS)]
    w_edges = [edges_out(2, k) for k in range(PARTS)]

    def fix_of(k):
        edges = z_recv[1, k]

        def step(n, held):
            planes = []
            for j in range(TOGETHER):
                i = TOGETHER * n + j
                x = DEEP * k + i
                a, near = neighbour_sum(res, x + 1, edges, i)
                planes.append([g[x + 1, h, MID, :] + (a[h] + near[h] * INV_DIAG) * INV_DIAG for h in range(2)])
                for h in range(2):
                    w[x + 1, h, MID, :] = planes[j][h]
            return pack_edges(planes, TOGETHER * n, held)

        return step

    for k in ORDER:
        if k in res_planes:
            res_planes[PARTS - 1 - k].wait_recv()
        for copy in res_rows[k] + [res_edges[k]]:
            copy.wait_recv()
        z_send[2, k] = lax.fori_loop(0, DEEP // TOGETHER, fix_of(k), zero)
        if k in w_planes:
            w_planes[k].start()
        start(w_rows[k])
        w_edges[k].start()

    def before_of(k):
        edges = z_recv[2, k]

        def step(n, carry):
            for j in range(TOGETHER):
                i = TOGETHER * n + j
                x = DEEP * k + i
                a, near = neighbour_sum(w, x + 1, edges, i)
                for h in range(2):
                    rs[x, h] = rs[x, h] - (DIAG * a[h] - near[h])
            return carry

        return step

    for k in ORDER:
        if k in w_planes:
            w_planes[PARTS - 1 - k].wait_recv()
        for copy in w_rows[k] + [w_edges[k]]:
            copy.wait_recv()
        lax.fori_loop(0, DEEP // TOGETHER, before_of(k), 0)

    others(lambda t: wait_recv(copy_c(t, t)))

    group_e = iota((EXTRA, 128), 1) // KZ

    def gather(X):
        out, out_e = jnp.zeros((CY, 128), F32), jnp.zeros((EXTRA, 128), F32)
        for t in range(GROUP):
            place = lax.rem(X + t, CX)
            out = jnp.where(group == place, c_recv[t], out)
            out_e = jnp.where(group_e == place, ce_recv[t], out_e)
        turn = lax.rem(128 - KZ * X + 128, 128)
        basis[X + 1, 0:CY, :] = pltpu.roll(out, turn, 1)
        basis[X + 1, CY : CY + EXTRA, :] = pltpu.roll(out_e, turn, 1)

    def gather_step(i, carry):
        gather(2 * i)
        gather(2 * i + 1)
        return carry

    lax.fori_loop(0, CX // 2, gather_step, 0)
    spot = iota((CY, 128), 1) // KZ
    for side, X in ((0, 0), (1, CX + 1)):
        out = jnp.zeros((CY, 128), F32)
        for t in range(GROUP):
            line = jnp.where(diagonal, ce_recv[t, 2 + side : 3 + side, :], 0.0)
            for move in (8, 16, 32, 64):
                line = line + pltpu.roll(line, move, 1)
            out = jnp.where(spot == t, line, out)
        basis[X, 0:CY, :] = out
        basis[X, CY:, :] = jnp.zeros((ROWS - CY, 128), F32)

    pz[...] = dot_right(basis[...].reshape((CX + 2) * ROWS, NC), iz).reshape(CX + 2, ROWS, 2 * BZ)

    def put(ref, X, h, four):
        for a in range(4):
            ref[X, h, pl.ds(a, CY, stride=4), :] = four[a]

    for X in (0, CX + 1):
        for h in range(2):
            put(corr, X, h, [pz[X, 0:CY, 128 * h : 128 * (h + 1)]] * 4)

    def prolong(X, carry):
        row = iota((CY, 128), 0)
        for h in range(2):
            lanes = slice(128 * h, 128 * (h + 1))
            here = pz[X, 0:CY, lanes]
            base = pz[X, 0:CY, BZ + 128 * h : BZ + 128 * (h + 1)]
            below = jnp.where(row == 0, pz[X, CY : CY + 1, lanes], pltpu.roll(here, 1, 0))
            above = jnp.where(row == CY - 1, pz[X, CY + 1 : CY + 2, lanes], pltpu.roll(here, CY - 1, 0))
            put(corr, X, h, [here] * 4)
            put(shift, X - 1, h, [base + (here - below), base, base, base + (here - above)])
        return carry

    lax.fori_loop(1, CX + 1, prolong, 0)

    def finish(X, total):
        for h in range(2):
            here = corr[X + 1, h]
            within = shift[X, h]
            low = here - corr[X, h]
            high = here - corr[X + 2, h]
            for j in range(4):
                x = 4 * X + j
                lanes = slice(128 * h, 128 * (h + 1))
                up_ref[x, :, lanes] = w[x + 1, h, MID, :] + here
                out = rs[x, h] - within
                if j == 0:
                    out = out - low
                if j == 3:
                    out = out - high
                new_ref[x, :, lanes] = out
                total = total + (out * out).reshape(8, 8, 128).sum(axis=0)
        return total

    total = lax.fori_loop(0, CX, finish, jnp.zeros((8, 128), F32))

    one = pl.ds(0, 1)
    n_send[...] = jnp.broadcast_to(jnp.sum(total, axis=0, keepdims=True), (8, 128))

    def copy_n(t, slot):
        return remote(n_send.at[one], n_recv.at[slot, one], n_ss.at[t], n_rs.at[slot], of_group(t))

    others(lambda t: copy_n(t, me).start())
    n_recv[me, 0:1, :] = n_send[0:1, :]
    others(lambda t: copy_n(t, t).wait_recv())
    total = n_recv[0, 0:1, :]
    for t in range(1, GROUP):
        total = total + n_recv[t, 0:1, :]
    n_held[0:1, :] = total

    def copy_l(d):
        to, slot = lax.rem(bx + d, GX), lax.rem(bx + GX - d, GX)
        return (
            remote(n_held.at[one], n_last.at[bx, one], l_ss.at[d], l_rs.at[bx], {"gx": to}),
            remote(n_held.at[one], n_last.at[slot, one], l_ss.at[d], l_rs.at[slot], {"gx": to}),
        )

    line = [copy_l(d) for d in range(1, GX)]
    for out, _ in line:
        out.start()
    n_last[bx, 0:1, :] = total
    for _, back in line:
        back.wait_recv()
    total = n_last[0, 0:1, :]
    for b in range(1, GX):
        total = total + n_last[b, 0:1, :]
    norm_ref[...] = jnp.sqrt(jnp.full((8, 128), jnp.sum(total), F32))

    for copy in list(g_planes.values()) + list(res_planes.values()) + list(w_planes.values()):
        copy.wait_send()
    for copies in g_rows + res_rows + w_rows + [g_edges, res_edges, w_edges, m_copies, v_copies]:
        for copy in copies:
            copy.wait_send()

    def all_sent(t):
        wait_send(copy_a(t, t))
        wait_send(copy_c(t, t))
        copy_n(t, t).wait_send()

    others(all_sent)
    for out, _ in line:
        out.wait_send()


ANY = pl.BlockSpec(memory_space=pl.ANY)
IN_VMEM = pl.BlockSpec(memory_space=pltpu.VMEM)
DMA = pltpu.SemaphoreType.DMA
VMEM = pltpu.VMEM


def per_device(right_side, guess):
    shape = jax.ShapeDtypeStruct
    block = (BX, BY, BZ)
    padded = (BX + 2, 2, PADDED, 128)
    updated, new_residual, norm = pl.pallas_call(
        kernel,
        out_shape=(shape(block, F32), shape(block, F32), shape((8, 128), F32)),
        in_specs=[ANY] * 2,
        out_specs=(IN_VMEM,) * 3,
        scratch_shapes=[
            VMEM(padded, F32), VMEM((BX, 2, BY, 128), F32), VMEM(padded, F32), VMEM(padded, F32),
            VMEM((2, 2 * BZ, NC), BF16), VMEM((2, NC, 2 * BZ), BF16), VMEM((2, NC, NC), BF16),
            VMEM((2, NC, GY * EXTRA), BF16), VMEM((2, GY * EXTRA, NC), BF16),
            VMEM((4, BY, 128), F32), VMEM((CX, CY, 2 * BZ), F32), VMEM((2, 4 * CX, 128), F32),
            VMEM((CX, CY, 128), F32), VMEM((GROUP, CY, 128), F32), VMEM((GROUP, CY, 128), F32),
            VMEM((GROUP, EXTRA, 128), F32), VMEM((GROUP, EXTRA, 128), F32), VMEM((GY * EXTRA, 128), F32),
            VMEM((CX, 128), F32), VMEM((GX, CX, 128), F32), VMEM((CX, 128), F32), VMEM((2, CX, 128), F32),
            VMEM((GY, CY, 128), F32), VMEM((GROUP, CY, 128), F32),
            VMEM((GY, EXTRA, 128), F32), VMEM((GROUP, EXTRA, 128), F32),
            VMEM((3, PARTS, 16, 128), F32), VMEM((3, PARTS, 16, 128), F32),
            VMEM((CX + 2, ROWS, 128), F32), VMEM((CX + 2, ROWS, 2 * BZ), F32),
            VMEM((CX + 2, 2, BY, 128), F32), VMEM((CX, 2, BY, 128), F32),
            VMEM((8, 128), F32), VMEM((GROUP, 8, 128), F32), VMEM((8, 128), F32), VMEM((GX, 8, 128), F32),
            DMA((LOADS, 2)), DMA((LOADS, 2)), DMA((2,)), DMA((2,)),
            DMA((3, 2)), DMA((3, 2)), DMA((3, PARTS, 2)), DMA((3, PARTS, 2)),
            DMA((3, PARTS)), DMA((3, PARTS)), DMA((GROUP,)), DMA((GROUP,)), DMA((GX,)), DMA((GX,)),
            DMA((GROUP,)), DMA((GROUP,)), DMA((GROUP,)), DMA((GROUP,)), DMA((GROUP,)), DMA((GROUP,)),
            DMA((GROUP,)), DMA((GROUP,)), DMA((GX,)), DMA((GX,)),
        ],
        compiler_params=pltpu.CompilerParams(
            collective_id=0, has_side_effects=True, vmem_limit_bytes=44 * 1024 * 1024
        ),
        name="schwarz",
    )(right_side, guess)
    return updated, new_residual, norm[0, 0]


def solution(mesh):
    spec = P("gx", "gy", "gz")
    return jax.shard_map(
        per_device, mesh=mesh, in_specs=(spec, spec), out_specs=(spec, spec, P()), check_vma=False
    )
```

```python
import math

import jax
import jax.numpy as jnp
from jax import lax
from jax.experimental import pallas as pl
from jax.experimental.pallas import tpu as pltpu
from jax.sharding import PartitionSpec as P

F32 = jnp.float32
BF16 = jnp.bfloat16
MESH = pl.DeviceIdType.MESH

SCREEN = 0.002
DIAG = 6.0 + SCREEN
INV_DIAG = 1.0 / DIAG

BX, BY, BZ = 64, 64, 256
CX, CY, CZ = 16, 16, 64
NC = 128
GX, GY, GZ = 8, 8, 2
GROUP = GY * GZ
KZ = NC // GROUP
EXTRA = 4
ROWS = 24
LOADS = 8
PLANES = BX // LOADS
PARTS = 4
DEEP = BX // PARTS
TOGETHER = 8
ORDER = (0, 3, 1, 2)
TOP = 8
PADDED = BY + 16
LOW, MID, HIGH = pl.ds(TOP - 1, BY), pl.ds(TOP, BY), pl.ds(TOP + 1, BY)


def sine(t):
    a = t.astype(F32) * (math.pi / 128.0)
    b = a * a
    p = -1.0 / 39916800.0
    for c in (1.0 / 362880.0, -1.0 / 5040.0, 1.0 / 120.0, -1.0 / 6.0, 1.0):
        p = p * b + c
    return a * p


def cas(product_of_indices):
    half = sine(jnp.abs(((product_of_indices - 16) & (NC - 1)) - 64))
    return math.sqrt(2.0) * (2.0 * half * half - 1.0)


def wave_of(k):
    half = sine(64 - jnp.abs(k - 64))
    return 4.0 * half * half


def split(a):
    high = a.astype(BF16)
    return high, (a - high.astype(F32)).astype(BF16)


def product(a, b):
    return jnp.dot(a, b, preferred_element_type=F32)


def dot_right(a, table):
    high, low = split(a)
    return product(high, table[0]) + (product(high, table[1]) + product(low, table[0]))


def dot_left(table, b):
    high, low = split(b)
    return product(table[0], high) + (product(table[0], low) + product(table[1], high))


def iota(shape, dim):
    return lax.broadcasted_iota(jnp.int32, shape, dim)


def mod(a, b):
    return a % b if isinstance(a, int) else lax.rem(a, b)


def neighbour_sum(ref, p, edges, i):
    lane = iota((BY, 128), 1)
    first, last = lane == 0, lane == 127
    a0, a1 = ref[p, 0, MID, :], ref[p, 1, MID, :]
    edge = jnp.concatenate([pltpu.roll(edges, 127 - 32 * q - 2 * i, 1) for q in range(4)], axis=0)
    up0, up1 = pltpu.roll(a0, 1, 1), pltpu.roll(a1, 1, 1)
    down0, down1 = pltpu.roll(a0, 127, 1), pltpu.roll(a1, 127, 1)
    sums = (
        jnp.where(first, edge, up0) + jnp.where(last, down1, down0),
        jnp.where(first, up0, up1) + jnp.where(last, edge, down1),
    )
    sums = tuple(
        s + ((ref[p - 1, h, MID, :] + ref[p + 1, h, MID, :]) + (ref[p, h, LOW, :] + ref[p, h, HIGH, :]))
        for h, s in enumerate(sums)
    )
    return (a0, a1), sums


def pack_edges(planes, i, held):
    lane = iota((16, 128), 1)
    end = lane == 127
    for j in range(len(planes) + 1):
        for q in range(4):
            rows = slice(16 * q, 16 * (q + 1))
            place = 32 * q + 2 * (i + j)
            if j == 0:
                value, mask = planes[0][0][rows], lane == place
            elif j == len(planes):
                value, mask = planes[-1][1][rows], lane == place - 1
            else:
                value = jnp.where(end, planes[j - 1][1][rows], planes[j][0][rows])
                mask = (lane == place) | (lane == place - 1)
            held = jnp.where(mask, pltpu.roll(value, mod(place, 128), 1), held)
    return held


def spread_lanes(a):
    a = jnp.where(iota(a.shape, 1) < KZ, a, 0.0)
    for shift in (8, 16, 32, 64):
        a = a + pltpu.roll(a, shift, 1)
    return a


def kernel(
    rs_hbm, g_hbm,
    up_ref, new_ref, norm_ref,
    g, rs, res, w, fz, iz, py, fe, ie,
    fold, folded, extra, spec, a_send, a_recv, ae_send, ae_recv, lines_e, m_send, m_recv, v_send, v_recv, c_send, c_recv, ce_send, ce_recv,
    z_send, z_recv, basis, pz, corr, shift, n_send, n_recv, n_held, n_last,
    g_sem, rs_sem, v_ss, v_rs, x_ss, x_rs, y_ss, y_rs, z_ss, z_rs, a_ss, a_rs, m_ss, m_rs, c_ss, c_rs, ae_ss, ae_rs, ce_ss, ce_rs,
    n_ss, n_rs, l_ss, l_rs,
):
    bx, by, bz = lax.axis_index("gx"), lax.axis_index("gy"), lax.axis_index("gz")
    me = bz * GY + by
    up_x, down_x = {"gx": lax.rem(bx + 1, GX)}, {"gx": lax.rem(bx + GX - 1, GX)}
    up_y, down_y = {"gy": lax.rem(by + 1, GY)}, {"gy": lax.rem(by + GY - 1, GY)}

    def of_group(t):
        return {"gy": lax.rem(t, GY), "gz": t // GY}

    def remote(src, dst, send, recv, where):
        return pltpu.make_async_remote_copy(src, dst, send, recv, device_id=where, device_id_type=MESH)

    def others(body):
        def across(d, carry):
            body((1 - bz) * GY + lax.rem(by + d, GY))
            return carry

        def along(d, carry):
            body(bz * GY + lax.rem(by + d, GY))
            return carry

        lax.fori_loop(0, GY, across, 0)
        lax.fori_loop(1, GY, along, 0)

    barrier = pltpu.get_barrier_semaphore()

    def greet(where):
        pl.semaphore_signal(barrier, inc=1, device_id=where, device_id_type=MESH)

    for d in range(1, GX):
        greet({"gx": lax.rem(bx + d, GX)})
    others(lambda t: greet(of_group(t)))

    halves = [pl.ds(0, 128), pl.ds(128, 128)]
    load_g = [
        [
            pltpu.make_async_copy(
                g_hbm.at[pl.ds(PLANES * c, PLANES), :, halves[h]],
                g.at[pl.ds(PLANES * c + 1, PLANES), h, MID, :],
                g_sem.at[c, h],
            )
            for h in range(2)
        ]
        for c in range(LOADS)
    ]
    load_rs = [
        [
            pltpu.make_async_copy(
                rs_hbm.at[pl.ds(PLANES * c, PLANES), :, halves[h]],
                rs.at[pl.ds(PLANES * c, PLANES), h],
                rs_sem.at[c, h],
            )
            for h in range(2)
        ]
        for c in range(LOADS)
    ]
    def start(copies):
        for copy in copies:
            copy.start()

    def wait(copies):
        for copy in copies:
            copy.wait()

    def wait_recv(copies):
        for copy in copies:
            copy.wait_recv()

    def wait_send(copies):
        for copy in copies:
            copy.wait_send()

    start(load_g[0])
    start(load_g[LOADS - 1])
    start(load_rs[0])
    for c in range(1, LOADS - 1):
        start(load_g[c])
        start(load_rs[c])
    start(load_rs[LOADS - 1])

    def keep(ref, rows, lanes, value):
        high, low = split(value)
        ref[0, rows, lanes] = high
        ref[1, rows, lanes] = low

    def beside(z):
        cell = CZ * bz + z // 4
        return cell, cell + jnp.where(z % 4 == 3, 1, 0) - jnp.where(z % 4 == 0, 1, 0)

    whole = slice(None)
    for part in range(4):
        cell, near = beside(iota((64, NC), 0) + 64 * part)
        mode = iota((64, NC), 1)
        here = cas(cell * mode)
        keep(fz, slice(64 * part, 64 * (part + 1)), whole, here)
        keep(fz, slice(BZ + 64 * part, BZ + 64 * (part + 1)), whole, cas(near * mode) - here)
    for part in range(2):
        cell, near = beside(iota((NC, 128), 1) + 128 * part)
        mode = iota((NC, 128), 0)
        here = cas(cell * mode)
        keep(iz, whole, slice(128 * part, 128 * (part + 1)), here)
        keep(iz, whole, slice(BZ + 128 * part, BZ + 128 * (part + 1)), SCREEN * here - (cas(near * mode) - here))

    keep(py, whole, whole, cas(iota((NC, NC), 0) * iota((NC, NC), 1)))

    def place_of(index):
        e = index % EXTRA
        return CY * (index // EXTRA) + jnp.where(e == 0, -1, CY), e < 2

    place, used = place_of(iota((NC, GY * EXTRA), 1))
    keep(fe, whole, whole, jnp.where(used, cas(place * iota((NC, GY * EXTRA), 0)), 0.0))
    place, used = place_of(iota((GY * EXTRA, NC), 0))
    keep(ie, whole, whole, jnp.where(used, cas(place * iota((GY * EXTRA, NC), 1)), 0.0))

    wait(load_g[0])
    wait(load_g[LOADS - 1])

    def every_fourth(ref, base):
        return [ref[pl.ds(base + a, 16, stride=4), :] for a in range(4)]

    def total_of(four):
        return (four[0] + four[1]) + (four[2] + four[3])

    for h in range(2):
        extra[h, 2 * CX : 3 * CX, :] = total_of(every_fourth(g.at[1, h], TOP))
        extra[h, 3 * CX :, :] = total_of(every_fourth(g.at[BX, h], TOP))

    def planes_out(phase, array):
        return {
            0: remote(
                array.at[1, :, MID, :], array.at[BX + 1, :, MID, :],
                x_ss.at[phase, 0], x_rs.at[phase, 0], down_x,
            ),
            PARTS - 1: remote(
                array.at[BX, :, MID, :], array.at[0, :, MID, :], x_ss.at[phase, 1], x_rs.at[phase, 1], up_x
            ),
        }

    def rows_out(phase, array, k):
        part = pl.ds(1 + DEEP * k, DEEP)
        return [
            remote(
                array.at[part, :, pl.ds(TOP, 1), :], array.at[part, :, pl.ds(TOP + BY, 1), :],
                y_ss.at[phase, k, 0], y_rs.at[phase, k, 0], down_y,
            ),
            remote(
                array.at[part, :, pl.ds(TOP + BY - 1, 1), :], array.at[part, :, pl.ds(TOP - 1, 1), :],
                y_ss.at[phase, k, 1], y_rs.at[phase, k, 1], up_y,
            ),
        ]

    def edges_out(phase, k):
        return remote(
            z_send.at[phase, k], z_recv.at[phase, k], z_ss.at[phase, k], z_rs.at[phase, k], {"gz": 1 - bz}
        )

    z_send[0] = jnp.zeros((PARTS, 16, 128), F32)

    def fold_plane(X, has_below=True, has_above=True):
        x = 4 * X + 1
        planes = []
        for j in range(4):
            planes.append((g[x + j, 0, MID, :], g[x + j, 1, MID, :]))
        for h in range(2):
            first, last = planes[0][h], planes[3][h]
            plane = (first + planes[1][h]) + (planes[2][h] + last)
            rest = (rs[x - 1, h] + rs[x, h]) + (rs[x + 1, h] + rs[x + 2, h])
            rest = rest - SCREEN * plane - (first + last)
            if has_below:
                rest = rest + g[x - 1, h, MID, :]
            if has_above:
                rest = rest + g[x + 4, h, MID, :]
            fold[h] = rest
            fold[2 + h] = plane
        rows = iota((CY, 128), 0)
        for h in range(2):
            a = every_fourth(fold.at[2 + h], 0)
            before = jnp.where(rows == 0, 0.0, pltpu.roll(a[3], 1, 0))
            after = jnp.where(rows == CY - 1, 0.0, pltpu.roll(a[0], CY - 1, 0))
            folded[X, :, 128 * h : 128 * (h + 1)] = (
                total_of(every_fourth(fold.at[h], 0)) + (before - a[0]) + (after - a[3])
            )
            folded[X, :, BZ + 128 * h : BZ + 128 * (h + 1)] = total_of(a)
            extra[h, pl.ds(X, 1), :] = fold[2 + h, 0:1, :]
            extra[h, pl.ds(CX + X, 1), :] = fold[2 + h, BY - 1 : BY, :]
        z_send[0, X // 4] = pack_edges(planes, 4 * mod(X, 4), z_send[0, X // 4])

    def fold_step(X, carry):
        fold_plane(X)
        return carry

    g_planes = planes_out(0, g)
    g_rows = [rows_out(0, g, k) for k in range(PARTS)]
    g_edges = [edges_out(0, k) for k in range(PARTS)]

    wait(load_rs[0])
    fold_plane(0, has_below=False)
    for c in range(1, LOADS - 1):
        wait(load_g[c])
        wait(load_rs[c])
        lax.fori_loop(2 * c - 1, 2 * c + 1, fold_step, 0)
        if c == 4:
            pl.semaphore_wait(barrier, GX - 1 + GROUP - 1)
            start(g_planes.values())
            for k in (0, 1):
                start(g_rows[k])
                g_edges[k].start()
    start(g_rows[2])
    g_edges[2].start()
    wait(load_rs[LOADS - 1])
    lax.fori_loop(CX - 3, CX - 1, fold_step, 0)
    fold_plane(CX - 1, has_above=False)
    start(g_rows[3])
    g_edges[3].start()

    spec[...] = dot_right(folded[...].reshape(CX * CY, 2 * BZ), fz).reshape(CX, CY, NC)
    more = dot_right(jnp.concatenate([extra[0], extra[1]], axis=1), fz.at[:, 0:BZ])
    for X in range(1, CX):
        spec[X] = pltpu.roll(spec[X], KZ * X, 1)
    row = iota((CY, 128), 0)
    group = iota((CY, 128), 1) // KZ
    sides = []
    for e in range(EXTRA):
        plane = more[CX * e : CX * (e + 1)]
        for bit in (1, 2, 4, 8):
            plane = jnp.where((row // bit) % 2 == 1, pltpu.roll(plane, KZ * bit, 1), plane)
        sides.append(plane)

    def message_a(t, ref, ref_e, slot):
        out = jnp.zeros((CY, 128), F32)
        for X in range(CX):
            out = jnp.where(group == lax.rem(t + X, CX), spec[X], out)
        ref[slot] = out
        turn = group == (row + t) % CX
        for e in range(EXTRA):
            ref_e[slot, e : e + 1, :] = jnp.sum(jnp.where(turn, sides[e], 0.0), axis=0, keepdims=True)

    def copy_a(t, slot):
        return (
            remote(a_send.at[t], a_recv.at[slot], a_ss.at[t], a_rs.at[slot], of_group(t)),
            remote(ae_send.at[t], ae_recv.at[slot], ae_ss.at[t], ae_rs.at[slot], of_group(t)),
        )

    def send_a(t):
        message_a(t, a_send, ae_send, t)
        start(copy_a(t, me))

    others(send_a)
    message_a(me, a_recv, ae_recv, me)
    place = iota((NC, 128), 1) // KZ
    wave = SCREEN * 16.0 + wave_of(iota((NC, 128), 0)) + wave_of(KZ * me + iota((NC, 128), 1) % KZ)
    r = 1.0 / (1.0 + 0.5 * wave + jnp.sqrt(wave + 0.25 * wave * wave))
    r2 = r * r
    r4 = r2 * r2
    r8 = r4 * r4
    r16 = r8 * r8
    inverse = 1.0 / r
    from_low, from_high = r, r
    for bit, power in ((1, r), (2, r2), (4, r4), (8, r8)):
        has = (place // bit) % 2 == 1
        from_low = from_low * jnp.where(has, power, 1.0)
        from_high = from_high * jnp.where(has, 1.0, power)

    res_planes = planes_out(1, res)
    res_rows = [rows_out(1, res, k) for k in range(PARTS)]
    res_edges = [edges_out(1, k) for k in range(PARTS)]

    def residual_of(k):
        edges = z_recv[0, k]

        def step(n, held):
            planes = []
            for j in range(TOGETHER):
                i = TOGETHER * n + j
                x = DEEP * k + i
                a, near = neighbour_sum(g, x + 1, edges, i)
                planes.append([rs[x, h] - (DIAG * a[h] - near[h]) for h in range(2)])
                for h in range(2):
                    res[x + 1, h, MID, :] = planes[j][h]
            return pack_edges(planes, TOGETHER * n, held)

        return step

    zero = jnp.zeros((16, 128), F32)
    for k in ORDER:
        if k in g_planes:
            g_planes[PARTS - 1 - k].wait_recv()
        for copy in g_rows[k] + [g_edges[k]]:
            copy.wait_recv()
        z_send[1, k] = lax.fori_loop(0, DEEP // TOGETHER, residual_of(k), zero)
        if k in res_planes:
            res_planes[k].start()
        start(res_rows[k])
        res_edges[k].start()

    others(lambda t: wait_recv(copy_a(t, t)))
    lines = (a_recv[0:GY] + a_recv[GY:GROUP]).reshape(NC, 128)
    turn = group == (row + me) % CX
    beyond = [[], []]
    for b in range(GY):
        four = ae_recv[b] + ae_recv[GY + b]
        lines_e[EXTRA * b : EXTRA * (b + 1), :] = four
        for side in range(2):
            beyond[side].append(jnp.where(turn, four[2 + side : 3 + side], 0.0))
    u = dot_left(py, lines) + dot_left(fe, lines_e[...])
    u = pltpu.roll(u, lax.rem(128 - KZ * me + 128, 128), 1)
    beyond = jnp.concatenate([jnp.concatenate(beyond[side], axis=0) for side in range(2)], axis=1)
    beyond = dot_left(py, beyond)
    out_low, out_high = beyond[:, :128], beyond[:, 128:]
    for move in (8, 16, 32, 64):
        out_low = out_low + pltpu.roll(out_low, move, 1)
        out_high = out_high + pltpu.roll(out_high, move, 1)

    right, left = u, u
    for step, power in ((1, r), (2, r2), (4, r4), (8, r8)):
        right = right + jnp.where(place >= step, power * pltpu.roll(right, KZ * step, 1), 0.0)
        left = left + jnp.where(place < CX - step, power * pltpu.roll(left, 128 - KZ * step, 1), 0.0)
    right = right + from_low * out_low
    left = left + from_high * out_high
    lane = iota((NC, 128), 1)
    outside = jnp.where(lane < KZ, out_low, out_high)
    ends = jnp.where(lane < KZ, left, pltpu.roll(right, 2 * KZ, 1)) + inverse * outside
    slot16 = iota((CX, 128), 1) // (2 * KZ)
    packed = jnp.zeros((CX, 128), F32)
    decay = jnp.zeros((CX, 128), F32)
    packed_out = jnp.zeros((CX, 128), F32)
    for i in range(8):
        part = ends[CX * i : CX * (i + 1)]
        packed = jnp.where(slot16 == i, pltpu.roll(part, 2 * KZ * i, 1) if i else part, packed)
        decay = jnp.where(slot16 == i, r16[CX * i : CX * (i + 1)], decay)
        part = outside[CX * i : CX * (i + 1)]
        packed_out = jnp.where(slot16 == i, pltpu.roll(part, 2 * KZ * i, 1) if i else part, packed_out)
    v_send[...] = packed_out
    m_send[...] = packed
    m_recv[0] = packed
    m_copies = [
        remote(m_send, m_recv.at[d], m_ss.at[d], m_rs.at[d], {"gx": lax.rem(bx + d, GX)}) for d in range(1, GX)
    ]
    start(m_copies)
    v_copies = [
        remote(v_send, v_recv.at[i], v_ss.at[i], v_rs.at[i], where) for i, where in enumerate((up_x, down_x))
    ]
    start(v_copies)

    end_left, end_right = spread_lanes(left), spread_lanes(pltpu.roll(right, KZ, 1))
    scale = (0.25 / (NC * NC)) * r / (1.0 - r2)
    local = right + left - u
    decay8 = decay * decay
    decay8 = decay8 * decay8
    decay8 = decay8 * decay8
    wrap = 1.0 / (1.0 - decay8)

    w_planes = planes_out(2, w)
    w_rows = [rows_out(2, w, k) for k in range(PARTS)]
    w_edges = [edges_out(2, k) for k in range(PARTS)]

    def fix_of(k):
        edges = z_recv[1, k]

        def step(n, held):
            planes = []
            for j in range(TOGETHER):
                i = TOGETHER * n + j
                x = DEEP * k + i
                a, near = neighbour_sum(res, x + 1, edges, i)
                planes.append([g[x + 1, h, MID, :] + (a[h] + near[h] * INV_DIAG) * INV_DIAG for h in range(2)])
                for h in range(2):
                    w[x + 1, h, MID, :] = planes[j][h]
            return pack_edges(planes, TOGETHER * n, held)

        return step

    def fix(parts):
        for k in parts:
            if k in res_planes:
                res_planes[PARTS - 1 - k].wait_recv()
            for copy in res_rows[k] + [res_edges[k]]:
                copy.wait_recv()
            z_send[2, k] = lax.fori_loop(0, DEEP // TOGETHER, fix_of(k), zero)
            if k in w_planes:
                w_planes[k].start()
            start(w_rows[k])
            w_edges[k].start()

    fix(ORDER)

    for copy in m_copies + v_copies:
        copy.wait_recv()
    is_right = (iota((CX, 128), 1) // KZ) % 2 == 1
    incoming = jnp.zeros((CX, 128), F32)
    for d in range(GX, 0, -1):
        incoming = jnp.where(is_right, m_recv[d % GX], m_recv[(GX - d) % GX]) + decay * incoming
    incoming = incoming * wrap

    def unpack(a):
        return jnp.concatenate(
            [pltpu.roll(a, 128 - 2 * KZ * i, 1) if i else a for i in range(8)], axis=0
        )

    unpacked = unpack(incoming)
    in_left, in_right = spread_lanes(unpacked), spread_lanes(pltpu.roll(unpacked, 128 - KZ, 1))
    near_out = unpack(jnp.where(is_right, v_recv[0], v_recv[1]))
    near_high, near_low = spread_lanes(near_out), spread_lanes(pltpu.roll(near_out, 128 - KZ, 1))
    solved = scale * (local + from_low * in_right + from_high * in_left)
    turned = r - inverse
    before = scale * (out_low + r * end_left + in_right + r16 * (r * in_left) + turned * near_low)
    after = scale * (out_high + r * end_right + in_left + r16 * (r * in_right) + turned * near_high)

    back = pltpu.roll(solved, KZ * me, 1)
    lines = dot_left(py, jnp.concatenate([back, before, after], axis=1))
    ends = dot_left(ie, back)
    diagonal = iota((CY, 128), 0) == iota((CY, 128), 1) // KZ
    for b in range(GY):
        rows = slice(CY * b, CY * (b + 1))
        c_send[b] = lines[rows, :128]
        ce_send[b, 0:2, :] = ends[EXTRA * b : EXTRA * b + 2]
        for side in range(2):
            plane = jnp.where(diagonal, lines[rows, 128 * (side + 1) : 128 * (side + 2)], 0.0)
            ce_send[b, 2 + side : 3 + side, :] = jnp.sum(plane, axis=0, keepdims=True)

    def copy_c(t, slot):
        b = lax.rem(t, GY)
        return (
            remote(c_send.at[b], c_recv.at[slot], c_ss.at[t], c_rs.at[slot], of_group(t)),
            remote(ce_send.at[b], ce_recv.at[slot], ce_ss.at[t], ce_rs.at[slot], of_group(t)),
        )

    others(lambda t: start(copy_c(t, me)))
    c_recv[me] = c_send[by]
    ce_recv[me] = ce_send[by]


    def before_of(k):
        edges = z_recv[2, k]

        def step(n, carry):
            for j in range(TOGETHER):
                i = TOGETHER * n + j
                x = DEEP * k + i
                a, near = neighbour_sum(w, x + 1, edges, i)
                for h in range(2):
                    rs[x, h] = rs[x, h] - (DIAG * a[h] - near[h])
            return carry

        return step

    for k in ORDER:
        if k in w_planes:
            w_planes[PARTS - 1 - k].wait_recv()
        for copy in w_rows[k] + [w_edges[k]]:
            copy.wait_recv()
        lax.fori_loop(0, DEEP // TOGETHER, before_of(k), 0)

    others(lambda t: wait_recv(copy_c(t, t)))

    group_e = iota((EXTRA, 128), 1) // KZ

    def gather(X):
        out, out_e = jnp.zeros((CY, 128), F32), jnp.zeros((EXTRA, 128), F32)
        for t in range(GROUP):
            place = lax.rem(X + t, CX)
            out = jnp.where(group == place, c_recv[t], out)
            out_e = jnp.where(group_e == place, ce_recv[t], out_e)
        turn = lax.rem(128 - KZ * X + 128, 128)
        basis[X + 1, 0:CY, :] = pltpu.roll(out, turn, 1)
        basis[X + 1, CY : CY + EXTRA, :] = pltpu.roll(out_e, turn, 1)

    def gather_step(i, carry):
        for j in range(4):
            gather(4 * i + j)
        return carry

    lax.fori_loop(0, CX // 4, gather_step, 0)
    spot = iota((CY, 128), 1) // KZ
    for side, X in ((0, 0), (1, CX + 1)):
        out = jnp.zeros((CY, 128), F32)
        for t in range(GROUP):
            line = jnp.where(diagonal, ce_recv[t, 2 + side : 3 + side, :], 0.0)
            for move in (8, 16, 32, 64):
                line = line + pltpu.roll(line, move, 1)
            out = jnp.where(spot == t, line, out)
        basis[X, 0:CY, :] = out
        basis[X, CY:, :] = jnp.zeros((ROWS - CY, 128), F32)

    pz[...] = dot_right(basis[...].reshape((CX + 2) * ROWS, NC), iz).reshape(CX + 2, ROWS, 2 * BZ)

    def put(ref, X, h, four):
        for a in range(4):
            ref[X, h, pl.ds(a, CY, stride=4), :] = four[a]

    for X in (0, CX + 1):
        for h in range(2):
            put(corr, X, h, [pz[X, 0:CY, 128 * h : 128 * (h + 1)]] * 4)

    def prolong(X, carry):
        row = iota((CY, 128), 0)
        for h in range(2):
            lanes = slice(128 * h, 128 * (h + 1))
            here = pz[X, 0:CY, lanes]
            base = pz[X, 0:CY, BZ + 128 * h : BZ + 128 * (h + 1)]
            below = jnp.where(row == 0, pz[X, CY : CY + 1, lanes], pltpu.roll(here, 1, 0))
            above = jnp.where(row == CY - 1, pz[X, CY + 1 : CY + 2, lanes], pltpu.roll(here, CY - 1, 0))
            put(corr, X, h, [here] * 4)
            put(shift, X - 1, h, [base + (here - below), base, base, base + (here - above)])
        return carry

    def by_two(body):
        return lambda i, carry: body(2 * i + 1, body(2 * i, carry))

    lax.fori_loop(0, CX // 2, by_two(lambda X, carry: prolong(X + 1, carry)), 0)

    def finish(X, total):
        for h in range(2):
            here = corr[X + 1, h]
            within = shift[X, h]
            low = here - corr[X, h]
            high = here - corr[X + 2, h]
            for j in range(4):
                x = 4 * X + j
                lanes = slice(128 * h, 128 * (h + 1))
                up_ref[x, :, lanes] = w[x + 1, h, MID, :] + here
                out = rs[x, h] - within
                if j == 0:
                    out = out - low
                if j == 3:
                    out = out - high
                new_ref[x, :, lanes] = out
                total = total + (out * out).reshape(8, 8, 128).sum(axis=0)
        return total

    total = lax.fori_loop(0, CX // 2, by_two(finish), jnp.zeros((8, 128), F32))

    one = pl.ds(0, 1)
    n_send[...] = jnp.broadcast_to(jnp.sum(total, axis=0, keepdims=True), (8, 128))

    def copy_n(t, slot):
        return remote(n_send.at[one], n_recv.at[slot, one], n_ss.at[t], n_rs.at[slot], of_group(t))

    others(lambda t: copy_n(t, me).start())
    n_recv[me, 0:1, :] = n_send[0:1, :]
    others(lambda t: copy_n(t, t).wait_recv())
    total = n_recv[0, 0:1, :]
    for t in range(1, GROUP):
        total = total + n_recv[t, 0:1, :]
    n_held[0:1, :] = total

    def copy_l(d):
        to, slot = lax.rem(bx + d, GX), lax.rem(bx + GX - d, GX)
        return (
            remote(n_held.at[one], n_last.at[bx, one], l_ss.at[d], l_rs.at[bx], {"gx": to}),
            remote(n_held.at[one], n_last.at[slot, one], l_ss.at[d], l_rs.at[slot], {"gx": to}),
        )

    line = [copy_l(d) for d in range(1, GX)]
    for out, _ in line:
        out.start()
    n_last[bx, 0:1, :] = total
    for _, back in line:
        back.wait_recv()
    total = n_last[0, 0:1, :]
    for b in range(1, GX):
        total = total + n_last[b, 0:1, :]
    norm_ref[...] = jnp.sqrt(jnp.full((8, 128), jnp.sum(total), F32))

    for copy in list(g_planes.values()) + list(res_planes.values()) + list(w_planes.values()):
        copy.wait_send()
    for copies in g_rows + res_rows + w_rows + [g_edges, res_edges, w_edges, m_copies, v_copies]:
        for copy in copies:
            copy.wait_send()

    def all_sent(t):
        wait_send(copy_a(t, t))
        wait_send(copy_c(t, t))
        copy_n(t, t).wait_send()

    others(all_sent)
    for out, _ in line:
        out.wait_send()


def hand_on(up, new, norm, up_hbm, new_hbm, norm_out, sems):
    part = BX // 2
    copies = [
        pltpu.make_async_copy(src.at[pl.ds(part * k, part)], dst.at[pl.ds(part * k, part)], sems.at[i, k])
        for k in range(2)
        for i, (src, dst) in enumerate(((up, up_hbm), (new, new_hbm)))
    ]
    for copy in copies:
        copy.start()
    norm_out[0, 0] = norm[0, 0]
    for copy in copies:
        copy.wait()


ANY = pl.BlockSpec(memory_space=pl.ANY)
IN_VMEM = pl.BlockSpec(memory_space=pltpu.VMEM)
DMA = pltpu.SemaphoreType.DMA
VMEM = pltpu.VMEM


def per_device(right_side, guess):
    shape = jax.ShapeDtypeStruct
    block = (BX, BY, BZ)
    padded = (BX + 2, 2, PADDED, 128)
    updated, new_residual, norm = pl.pallas_call(
        kernel,
        out_shape=(shape(block, F32), shape(block, F32), shape((8, 128), F32)),
        in_specs=[ANY] * 2,
        out_specs=(IN_VMEM,) * 3,
        scratch_shapes=[
            VMEM(padded, F32), VMEM((BX, 2, BY, 128), F32), VMEM(padded, F32), VMEM(padded, F32),
            VMEM((2, 2 * BZ, NC), BF16), VMEM((2, NC, 2 * BZ), BF16), VMEM((2, NC, NC), BF16),
            VMEM((2, NC, GY * EXTRA), BF16), VMEM((2, GY * EXTRA, NC), BF16),
            VMEM((4, BY, 128), F32), VMEM((CX, CY, 2 * BZ), F32), VMEM((2, 4 * CX, 128), F32),
            VMEM((CX, CY, 128), F32), VMEM((GROUP, CY, 128), F32), VMEM((GROUP, CY, 128), F32),
            VMEM((GROUP, EXTRA, 128), F32), VMEM((GROUP, EXTRA, 128), F32), VMEM((GY * EXTRA, 128), F32),
            VMEM((CX, 128), F32), VMEM((GX, CX, 128), F32), VMEM((CX, 128), F32), VMEM((2, CX, 128), F32),
            VMEM((GY, CY, 128), F32), VMEM((GROUP, CY, 128), F32),
            VMEM((GY, EXTRA, 128), F32), VMEM((GROUP, EXTRA, 128), F32),
            VMEM((3, PARTS, 16, 128), F32), VMEM((3, PARTS, 16, 128), F32),
            VMEM((CX + 2, ROWS, 128), F32), VMEM((CX + 2, ROWS, 2 * BZ), F32),
            VMEM((CX + 2, 2, BY, 128), F32), VMEM((CX, 2, BY, 128), F32),
            VMEM((8, 128), F32), VMEM((GROUP, 8, 128), F32), VMEM((8, 128), F32), VMEM((GX, 8, 128), F32),
            DMA((LOADS, 2)), DMA((LOADS, 2)), DMA((2,)), DMA((2,)),
            DMA((3, 2)), DMA((3, 2)), DMA((3, PARTS, 2)), DMA((3, PARTS, 2)),
            DMA((3, PARTS)), DMA((3, PARTS)), DMA((GROUP,)), DMA((GROUP,)), DMA((GX,)), DMA((GX,)),
            DMA((GROUP,)), DMA((GROUP,)), DMA((GROUP,)), DMA((GROUP,)), DMA((GROUP,)), DMA((GROUP,)),
            DMA((GROUP,)), DMA((GROUP,)), DMA((GX,)), DMA((GX,)),
        ],
        compiler_params=pltpu.CompilerParams(
            collective_id=0, has_side_effects=True, vmem_limit_bytes=44 * 1024 * 1024
        ),
        name="schwarz",
    )(right_side, guess)
    updated, new_residual, norm = pl.pallas_call(
        hand_on,
        out_shape=(shape(block, F32), shape(block, F32), shape((1, 1), F32)),
        in_specs=[ANY, ANY, IN_VMEM],
        out_specs=(ANY, ANY, pl.BlockSpec(memory_space=pltpu.SMEM)),
        scratch_shapes=[DMA((2, 2))],
        compiler_params=pltpu.CompilerParams(vmem_limit_bytes=1024 * 1024),
        name="hand_on",
    )(updated, new_residual, norm)
    return updated, new_residual, norm.reshape(())


def solution(mesh):
    spec = P("gx", "gy", "gz")
    return jax.shard_map(
        per_device, mesh=mesh, in_specs=(spec, spec), out_specs=(spec, spec, P()), check_vma=False
    )
```

```python
import math

import jax
import jax.numpy as jnp
from jax import lax
from jax.experimental import pallas as pl
from jax.experimental.pallas import tpu as pltpu
from jax.sharding import PartitionSpec as P

F32 = jnp.float32
BF16 = jnp.bfloat16
MESH = pl.DeviceIdType.MESH

SCREEN = 0.002
DIAG = 6.0 + SCREEN
INV_DIAG = 1.0 / DIAG

BX, BY, BZ = 64, 64, 256
CX, CY, CZ = 16, 16, 64
NC = 128
GX, GY, GZ = 8, 8, 2
GROUP = GY * GZ
KZ = NC // GROUP
EXTRA = 4
ROWS = 24
LOADS = 8
PLANES = BX // LOADS
PARTS = 4
DEEP = BX // PARTS
TOGETHER = 8
ORDER = (0, 3, 1, 2)
TOP = 8
PADDED = BY + 16
LOW, MID, HIGH = pl.ds(TOP - 1, BY), pl.ds(TOP, BY), pl.ds(TOP + 1, BY)


def sine(t):
    a = t.astype(F32) * (math.pi / 128.0)
    b = a * a
    p = -1.0 / 39916800.0
    for c in (1.0 / 362880.0, -1.0 / 5040.0, 1.0 / 120.0, -1.0 / 6.0, 1.0):
        p = p * b + c
    return a * p


def cas(product_of_indices):
    half = sine(jnp.abs(((product_of_indices - 16) & (NC - 1)) - 64))
    return math.sqrt(2.0) * (2.0 * half * half - 1.0)


def wave_of(k):
    half = sine(64 - jnp.abs(k - 64))
    return 4.0 * half * half


def split(a):
    high = a.astype(BF16)
    return high, (a - high.astype(F32)).astype(BF16)


def product(a, b):
    return jnp.dot(a, b, preferred_element_type=F32)


def dot_right(a, table):
    high, low = split(a)
    return product(high, table[0]) + (product(high, table[1]) + product(low, table[0]))


def dot_left(table, b):
    high, low = split(b)
    return product(table[0], high) + (product(table[0], low) + product(table[1], high))


def iota(shape, dim):
    return lax.broadcasted_iota(jnp.int32, shape, dim)


def mod(a, b):
    return a % b if isinstance(a, int) else lax.rem(a, b)


def neighbour_sum(ref, p, edges, i):
    lane = iota((BY, 128), 1)
    first, last = lane == 0, lane == 127
    a0, a1 = ref[p, 0, MID, :], ref[p, 1, MID, :]
    edge = jnp.concatenate([pltpu.roll(edges, 127 - 32 * q - 2 * i, 1) for q in range(4)], axis=0)
    up0, up1 = pltpu.roll(a0, 1, 1), pltpu.roll(a1, 1, 1)
    down0, down1 = pltpu.roll(a0, 127, 1), pltpu.roll(a1, 127, 1)
    sums = (
        jnp.where(first, edge, up0) + jnp.where(last, down1, down0),
        jnp.where(first, up0, up1) + jnp.where(last, edge, down1),
    )
    sums = tuple(
        s + ((ref[p - 1, h, MID, :] + ref[p + 1, h, MID, :]) + (ref[p, h, LOW, :] + ref[p, h, HIGH, :]))
        for h, s in enumerate(sums)
    )
    return (a0, a1), sums


def pack_edges(planes, i, held):
    lane = iota((16, 128), 1)
    end = lane == 127
    for j in range(len(planes) + 1):
        for q in range(4):
            rows = slice(16 * q, 16 * (q + 1))
            place = 32 * q + 2 * (i + j)
            if j == 0:
                value, mask = planes[0][0][rows], lane == place
            elif j == len(planes):
                value, mask = planes[-1][1][rows], lane == place - 1
            else:
                value = jnp.where(end, planes[j - 1][1][rows], planes[j][0][rows])
                mask = (lane == place) | (lane == place - 1)
            held = jnp.where(mask, pltpu.roll(value, mod(place, 128), 1), held)
    return held


def spread_lanes(a):
    a = jnp.where(iota(a.shape, 1) < KZ, a, 0.0)
    for shift in (8, 16, 32, 64):
        a = a + pltpu.roll(a, shift, 1)
    return a


def kernel(
    rs_hbm, g_hbm,
    up_ref, new_ref, norm_ref,
    g, rs, res, w, fz, iz, py, fe, ie,
    fold, folded, extra, spec, a_send, a_recv, ae_send, ae_recv, lines_e, m_send, m_recv, v_send, v_recv, c_send, c_recv, ce_send, ce_recv,
    z_send, z_recv, basis, pz, corr, shift, n_send, n_recv, n_held, n_last,
    g_sem, rs_sem, v_ss, v_rs, x_ss, x_rs, y_ss, y_rs, z_ss, z_rs, a_ss, a_rs, m_ss, m_rs, c_ss, c_rs, ae_ss, ae_rs, ce_ss, ce_rs,
    n_ss, n_rs, l_ss, l_rs,
):
    bx, by, bz = lax.axis_index("gx"), lax.axis_index("gy"), lax.axis_index("gz")
    me = bz * GY + by
    up_x, down_x = {"gx": lax.rem(bx + 1, GX)}, {"gx": lax.rem(bx + GX - 1, GX)}
    up_y, down_y = {"gy": lax.rem(by + 1, GY)}, {"gy": lax.rem(by + GY - 1, GY)}

    def of_group(t):
        return {"gy": lax.rem(t, GY), "gz": t // GY}

    def remote(src, dst, send, recv, where):
        return pltpu.make_async_remote_copy(src, dst, send, recv, device_id=where, device_id_type=MESH)

    def others(body):
        def across(d, carry):
            body((1 - bz) * GY + lax.rem(by + d, GY))
            return carry

        def along(d, carry):
            body(bz * GY + lax.rem(by + d, GY))
            return carry

        lax.fori_loop(0, GY, across, 0)
        lax.fori_loop(1, GY, along, 0)

    barrier = pltpu.get_barrier_semaphore()

    def greet(where):
        pl.semaphore_signal(barrier, inc=1, device_id=where, device_id_type=MESH)

    for d in range(1, GX):
        greet({"gx": lax.rem(bx + d, GX)})
    others(lambda t: greet(of_group(t)))

    halves = [pl.ds(0, 128), pl.ds(128, 128)]
    load_g = [
        [
            pltpu.make_async_copy(
                g_hbm.at[pl.ds(PLANES * c, PLANES), :, halves[h]],
                g.at[pl.ds(PLANES * c + 1, PLANES), h, MID, :],
                g_sem.at[c, h],
            )
            for h in range(2)
        ]
        for c in range(LOADS)
    ]
    load_rs = [
        [
            pltpu.make_async_copy(
                rs_hbm.at[pl.ds(PLANES * c, PLANES), :, halves[h]],
                rs.at[pl.ds(PLANES * c, PLANES), h],
                rs_sem.at[c, h],
            )
            for h in range(2)
        ]
        for c in range(LOADS)
    ]
    def start(copies):
        for copy in copies:
            copy.start()

    def wait(copies):
        for copy in copies:
            copy.wait()

    def wait_recv(copies):
        for copy in copies:
            copy.wait_recv()

    def wait_send(copies):
        for copy in copies:
            copy.wait_send()

    start(load_g[0])
    start(load_g[LOADS - 1])
    start(load_rs[0])
    for c in range(1, LOADS - 1):
        start(load_g[c])
        start(load_rs[c])
    start(load_rs[LOADS - 1])

    def keep(ref, rows, lanes, value):
        high, low = split(value)
        ref[0, rows, lanes] = high
        ref[1, rows, lanes] = low

    def beside(z):
        cell = CZ * bz + z // 4
        return cell, cell + jnp.where(z % 4 == 3, 1, 0) - jnp.where(z % 4 == 0, 1, 0)

    whole = slice(None)
    for part in range(4):
        cell, near = beside(iota((64, NC), 0) + 64 * part)
        mode = iota((64, NC), 1)
        here = cas(cell * mode)
        keep(fz, slice(64 * part, 64 * (part + 1)), whole, here)
        keep(fz, slice(BZ + 64 * part, BZ + 64 * (part + 1)), whole, cas(near * mode) - here)
    for part in range(2):
        cell, near = beside(iota((NC, 128), 1) + 128 * part)
        mode = iota((NC, 128), 0)
        here = cas(cell * mode)
        keep(iz, whole, slice(128 * part, 128 * (part + 1)), here)
        keep(iz, whole, slice(BZ + 128 * part, BZ + 128 * (part + 1)), SCREEN * here - (cas(near * mode) - here))

    keep(py, whole, whole, cas(iota((NC, NC), 0) * iota((NC, NC), 1)))

    def place_of(index):
        e = index % EXTRA
        return CY * (index // EXTRA) + jnp.where(e == 0, -1, CY), e < 2

    place, used = place_of(iota((NC, GY * EXTRA), 1))
    keep(fe, whole, whole, jnp.where(used, cas(place * iota((NC, GY * EXTRA), 0)), 0.0))
    place, used = place_of(iota((GY * EXTRA, NC), 0))
    keep(ie, whole, whole, jnp.where(used, cas(place * iota((GY * EXTRA, NC), 1)), 0.0))

    wait(load_g[0])
    wait(load_g[LOADS - 1])

    def every_fourth(ref, base):
        return [ref[pl.ds(base + a, 16, stride=4), :] for a in range(4)]

    def total_of(four):
        return (four[0] + four[1]) + (four[2] + four[3])

    for h in range(2):
        extra[h, 2 * CX : 3 * CX, :] = total_of(every_fourth(g.at[1, h], TOP))
        extra[h, 3 * CX :, :] = total_of(every_fourth(g.at[BX, h], TOP))

    def planes_out(phase, array):
        return {
            0: remote(
                array.at[1, :, MID, :], array.at[BX + 1, :, MID, :],
                x_ss.at[phase, 0], x_rs.at[phase, 0], down_x,
            ),
            PARTS - 1: remote(
                array.at[BX, :, MID, :], array.at[0, :, MID, :], x_ss.at[phase, 1], x_rs.at[phase, 1], up_x
            ),
        }

    def rows_out(phase, array, k):
        part = pl.ds(1 + DEEP * k, DEEP)
        return [
            remote(
                array.at[part, :, pl.ds(TOP, 1), :], array.at[part, :, pl.ds(TOP + BY, 1), :],
                y_ss.at[phase, k, 0], y_rs.at[phase, k, 0], down_y,
            ),
            remote(
                array.at[part, :, pl.ds(TOP + BY - 1, 1), :], array.at[part, :, pl.ds(TOP - 1, 1), :],
                y_ss.at[phase, k, 1], y_rs.at[phase, k, 1], up_y,
            ),
        ]

    def edges_out(phase, k):
        return remote(
            z_send.at[phase, k], z_recv.at[phase, k], z_ss.at[phase, k], z_rs.at[phase, k], {"gz": 1 - bz}
        )

    z_send[0] = jnp.zeros((PARTS, 16, 128), F32)

    def fold_plane(X, has_below=True, has_above=True):
        x = 4 * X + 1
        planes = []
        for j in range(4):
            planes.append((g[x + j, 0, MID, :], g[x + j, 1, MID, :]))
        for h in range(2):
            first, last = planes[0][h], planes[3][h]
            plane = (first + planes[1][h]) + (planes[2][h] + last)
            rest = (rs[x - 1, h] + rs[x, h]) + (rs[x + 1, h] + rs[x + 2, h])
            rest = rest - SCREEN * plane - (first + last)
            if has_below:
                rest = rest + g[x - 1, h, MID, :]
            if has_above:
                rest = rest + g[x + 4, h, MID, :]
            fold[h] = rest
            fold[2 + h] = plane
        rows = iota((CY, 128), 0)
        for h in range(2):
            a = every_fourth(fold.at[2 + h], 0)
            before = jnp.where(rows == 0, 0.0, pltpu.roll(a[3], 1, 0))
            after = jnp.where(rows == CY - 1, 0.0, pltpu.roll(a[0], CY - 1, 0))
            folded[X, :, 128 * h : 128 * (h + 1)] = (
                total_of(every_fourth(fold.at[h], 0)) + (before - a[0]) + (after - a[3])
            )
            folded[X, :, BZ + 128 * h : BZ + 128 * (h + 1)] = total_of(a)
            extra[h, pl.ds(X, 1), :] = fold[2 + h, 0:1, :]
            extra[h, pl.ds(CX + X, 1), :] = fold[2 + h, BY - 1 : BY, :]
        z_send[0, X // 4] = pack_edges(planes, 4 * mod(X, 4), z_send[0, X // 4])

    def fold_step(X, carry):
        fold_plane(X)
        return carry

    g_planes = planes_out(0, g)
    g_rows = [rows_out(0, g, k) for k in range(PARTS)]
    g_edges = [edges_out(0, k) for k in range(PARTS)]

    wait(load_rs[0])
    fold_plane(0, has_below=False)
    for c in range(1, LOADS - 1):
        wait(load_g[c])
        wait(load_rs[c])
        lax.fori_loop(2 * c - 1, 2 * c + 1, fold_step, 0)
        if c == 4:
            pl.semaphore_wait(barrier, GX - 1 + GROUP - 1)
            start(g_planes.values())
            for k in (0, 1):
                start(g_rows[k])
                g_edges[k].start()
    start(g_rows[2])
    g_edges[2].start()
    wait(load_rs[LOADS - 1])
    lax.fori_loop(CX - 3, CX - 1, fold_step, 0)
    fold_plane(CX - 1, has_above=False)
    start(g_rows[3])
    g_edges[3].start()

    spec[...] = dot_right(folded[...].reshape(CX * CY, 2 * BZ), fz).reshape(CX, CY, NC)
    more = dot_right(jnp.concatenate([extra[0], extra[1]], axis=1), fz.at[:, 0:BZ])
    for X in range(1, CX):
        spec[X] = pltpu.roll(spec[X], KZ * X, 1)
    row = iota((CY, 128), 0)
    group = iota((CY, 128), 1) // KZ
    sides = []
    for e in range(EXTRA):
        plane = more[CX * e : CX * (e + 1)]
        for bit in (1, 2, 4, 8):
            plane = jnp.where((row // bit) % 2 == 1, pltpu.roll(plane, KZ * bit, 1), plane)
        sides.append(plane)

    def message_a(t, ref, ref_e, slot):
        out = jnp.zeros((CY, 128), F32)
        for X in range(CX):
            out = jnp.where(group == lax.rem(t + X, CX), spec[X], out)
        ref[slot] = out
        turn = group == (row + t) % CX
        for e in range(EXTRA):
            ref_e[slot, e : e + 1, :] = jnp.sum(jnp.where(turn, sides[e], 0.0), axis=0, keepdims=True)

    def copy_a(t, slot):
        return (
            remote(a_send.at[t], a_recv.at[slot], a_ss.at[t], a_rs.at[slot], of_group(t)),
            remote(ae_send.at[t], ae_recv.at[slot], ae_ss.at[t], ae_rs.at[slot], of_group(t)),
        )

    def send_a(t):
        message_a(t, a_send, ae_send, t)
        start(copy_a(t, me))

    others(send_a)
    message_a(me, a_recv, ae_recv, me)
    place = iota((NC, 128), 1) // KZ
    wave = SCREEN * 16.0 + wave_of(iota((NC, 128), 0)) + wave_of(KZ * me + iota((NC, 128), 1) % KZ)
    r = 1.0 / (1.0 + 0.5 * wave + jnp.sqrt(wave + 0.25 * wave * wave))
    r2 = r * r
    r4 = r2 * r2
    r8 = r4 * r4
    r16 = r8 * r8
    inverse = 1.0 / r
    from_low, from_high = r, r
    for bit, power in ((1, r), (2, r2), (4, r4), (8, r8)):
        has = (place // bit) % 2 == 1
        from_low = from_low * jnp.where(has, power, 1.0)
        from_high = from_high * jnp.where(has, 1.0, power)

    res_planes = planes_out(1, res)
    res_rows = [rows_out(1, res, k) for k in range(PARTS)]
    res_edges = [edges_out(1, k) for k in range(PARTS)]

    def residual_of(k):
        edges = z_recv[0, k]

        def step(n, held):
            planes = []
            for j in range(TOGETHER):
                i = TOGETHER * n + j
                x = DEEP * k + i
                a, near = neighbour_sum(g, x + 1, edges, i)
                planes.append([rs[x, h] - (DIAG * a[h] - near[h]) for h in range(2)])
                for h in range(2):
                    res[x + 1, h, MID, :] = planes[j][h]
            return pack_edges(planes, TOGETHER * n, held)

        return step

    zero = jnp.zeros((16, 128), F32)
    for k in ORDER:
        if k in g_planes:
            g_planes[PARTS - 1 - k].wait_recv()
        for copy in g_rows[k] + [g_edges[k]]:
            copy.wait_recv()
        z_send[1, k] = lax.fori_loop(0, DEEP // TOGETHER, residual_of(k), zero)
        if k in res_planes:
            res_planes[k].start()
        start(res_rows[k])
        res_edges[k].start()

    others(lambda t: wait_recv(copy_a(t, t)))
    lines = (a_recv[0:GY] + a_recv[GY:GROUP]).reshape(NC, 128)
    turn = group == (row + me) % CX
    beyond = [[], []]
    for b in range(GY):
        four = ae_recv[b] + ae_recv[GY + b]
        lines_e[EXTRA * b : EXTRA * (b + 1), :] = four
        for side in range(2):
            beyond[side].append(jnp.where(turn, four[2 + side : 3 + side], 0.0))
    u = dot_left(py, lines) + dot_left(fe, lines_e[...])
    u = pltpu.roll(u, lax.rem(128 - KZ * me + 128, 128), 1)
    beyond = jnp.concatenate([jnp.concatenate(beyond[side], axis=0) for side in range(2)], axis=1)
    beyond = dot_left(py, beyond)
    out_low, out_high = beyond[:, :128], beyond[:, 128:]
    for move in (8, 16, 32, 64):
        out_low = out_low + pltpu.roll(out_low, move, 1)
        out_high = out_high + pltpu.roll(out_high, move, 1)

    right, left = u, u
    for step, power in ((1, r), (2, r2), (4, r4), (8, r8)):
        right = right + jnp.where(place >= step, power * pltpu.roll(right, KZ * step, 1), 0.0)
        left = left + jnp.where(place < CX - step, power * pltpu.roll(left, 128 - KZ * step, 1), 0.0)
    right = right + from_low * out_low
    left = left + from_high * out_high
    lane = iota((NC, 128), 1)
    outside = jnp.where(lane < KZ, out_low, out_high)
    ends = jnp.where(lane < KZ, left, pltpu.roll(right, 2 * KZ, 1)) + inverse * outside
    slot16 = iota((CX, 128), 1) // (2 * KZ)
    packed = jnp.zeros((CX, 128), F32)
    decay = jnp.zeros((CX, 128), F32)
    packed_out = jnp.zeros((CX, 128), F32)
    for i in range(8):
        part = ends[CX * i : CX * (i + 1)]
        packed = jnp.where(slot16 == i, pltpu.roll(part, 2 * KZ * i, 1) if i else part, packed)
        decay = jnp.where(slot16 == i, r16[CX * i : CX * (i + 1)], decay)
        part = outside[CX * i : CX * (i + 1)]
        packed_out = jnp.where(slot16 == i, pltpu.roll(part, 2 * KZ * i, 1) if i else part, packed_out)
    v_send[...] = packed_out
    m_send[...] = packed
    m_recv[0] = packed
    m_copies = [
        remote(m_send, m_recv.at[d], m_ss.at[d], m_rs.at[d], {"gx": lax.rem(bx + d, GX)}) for d in range(1, GX)
    ]
    start(m_copies)
    v_copies = [
        remote(v_send, v_recv.at[i], v_ss.at[i], v_rs.at[i], where) for i, where in enumerate((up_x, down_x))
    ]
    start(v_copies)

    end_left, end_right = spread_lanes(left), spread_lanes(pltpu.roll(right, KZ, 1))
    scale = (0.25 / (NC * NC)) * r / (1.0 - r2)
    local = right + left - u
    decay8 = decay * decay
    decay8 = decay8 * decay8
    decay8 = decay8 * decay8
    wrap = 1.0 / (1.0 - decay8)

    w_planes = planes_out(2, w)
    w_rows = [rows_out(2, w, k) for k in range(PARTS)]
    w_edges = [edges_out(2, k) for k in range(PARTS)]

    def fix_of(k):
        edges = z_recv[1, k]

        def step(n, held):
            planes = []
            for j in range(TOGETHER):
                i = TOGETHER * n + j
                x = DEEP * k + i
                a, near = neighbour_sum(res, x + 1, edges, i)
                planes.append([g[x + 1, h, MID, :] + (a[h] + near[h] * INV_DIAG) * INV_DIAG for h in range(2)])
                for h in range(2):
                    w[x + 1, h, MID, :] = planes[j][h]
            return pack_edges(planes, TOGETHER * n, held)

        return step

    def fix(parts):
        for k in parts:
            if k in res_planes:
                res_planes[PARTS - 1 - k].wait_recv()
            for copy in res_rows[k] + [res_edges[k]]:
                copy.wait_recv()
            z_send[2, k] = lax.fori_loop(0, DEEP // TOGETHER, fix_of(k), zero)
            if k in w_planes:
                w_planes[k].start()
            start(w_rows[k])
            w_edges[k].start()

    fix(ORDER)

    for copy in m_copies + v_copies:
        copy.wait_recv()
    is_right = (iota((CX, 128), 1) // KZ) % 2 == 1
    incoming = jnp.zeros((CX, 128), F32)
    for d in range(GX, 0, -1):
        incoming = jnp.where(is_right, m_recv[d % GX], m_recv[(GX - d) % GX]) + decay * incoming
    incoming = incoming * wrap

    def unpack(a):
        return jnp.concatenate(
            [pltpu.roll(a, 128 - 2 * KZ * i, 1) if i else a for i in range(8)], axis=0
        )

    unpacked = unpack(incoming)
    in_left, in_right = spread_lanes(unpacked), spread_lanes(pltpu.roll(unpacked, 128 - KZ, 1))
    near_out = unpack(jnp.where(is_right, v_recv[0], v_recv[1]))
    near_high, near_low = spread_lanes(near_out), spread_lanes(pltpu.roll(near_out, 128 - KZ, 1))
    solved = scale * (local + from_low * in_right + from_high * in_left)
    turned = r - inverse
    before = scale * (out_low + r * end_left + in_right + r16 * (r * in_left) + turned * near_low)
    after = scale * (out_high + r * end_right + in_left + r16 * (r * in_right) + turned * near_high)

    back = pltpu.roll(solved, KZ * me, 1)
    lines = dot_left(py, jnp.concatenate([back, before, after], axis=1))
    ends = dot_left(ie, back)
    diagonal = iota((CY, 128), 0) == iota((CY, 128), 1) // KZ
    for b in range(GY):
        rows = slice(CY * b, CY * (b + 1))
        c_send[b] = lines[rows, :128]
        ce_send[b, 0:2, :] = ends[EXTRA * b : EXTRA * b + 2]
        for side in range(2):
            plane = jnp.where(diagonal, lines[rows, 128 * (side + 1) : 128 * (side + 2)], 0.0)
            ce_send[b, 2 + side : 3 + side, :] = jnp.sum(plane, axis=0, keepdims=True)

    def copy_c(t, slot):
        b = lax.rem(t, GY)
        return (
            remote(c_send.at[b], c_recv.at[slot], c_ss.at[t], c_rs.at[slot], of_group(t)),
            remote(ce_send.at[b], ce_recv.at[slot], ce_ss.at[t], ce_rs.at[slot], of_group(t)),
        )

    others(lambda t: start(copy_c(t, me)))
    c_recv[me] = c_send[by]
    ce_recv[me] = ce_send[by]


    def before_of(k):
        edges = z_recv[2, k]

        def step(n, carry):
            for j in range(TOGETHER):
                i = TOGETHER * n + j
                x = DEEP * k + i
                a, near = neighbour_sum(w, x + 1, edges, i)
                for h in range(2):
                    rs[x, h] = rs[x, h] - (DIAG * a[h] - near[h])
            return carry

        return step

    for k in ORDER:
        if k in w_planes:
            w_planes[PARTS - 1 - k].wait_recv()
        for copy in w_rows[k] + [w_edges[k]]:
            copy.wait_recv()
        lax.fori_loop(0, DEEP // TOGETHER, before_of(k), 0)

    others(lambda t: wait_recv(copy_c(t, t)))

    group_e = iota((EXTRA, 128), 1) // KZ

    def gather(X):
        out, out_e = jnp.zeros((CY, 128), F32), jnp.zeros((EXTRA, 128), F32)
        for t in range(GROUP):
            place = lax.rem(X + t, CX)
            out = jnp.where(group == place, c_recv[t], out)
            out_e = jnp.where(group_e == place, ce_recv[t], out_e)
        turn = lax.rem(128 - KZ * X + 128, 128)
        basis[X + 1, 0:CY, :] = pltpu.roll(out, turn, 1)
        basis[X + 1, CY : CY + EXTRA, :] = pltpu.roll(out_e, turn, 1)

    def gather_step(i, carry):
        for j in range(4):
            gather(4 * i + j)
        return carry

    lax.fori_loop(0, CX // 4, gather_step, 0)
    spot = iota((CY, 128), 1) // KZ
    for side, X in ((0, 0), (1, CX + 1)):
        out = jnp.zeros((CY, 128), F32)
        for t in range(GROUP):
            line = jnp.where(diagonal, ce_recv[t, 2 + side : 3 + side, :], 0.0)
            for move in (8, 16, 32, 64):
                line = line + pltpu.roll(line, move, 1)
            out = jnp.where(spot == t, line, out)
        basis[X, 0:CY, :] = out
        basis[X, CY:, :] = jnp.zeros((ROWS - CY, 128), F32)

    pz[...] = dot_right(basis[...].reshape((CX + 2) * ROWS, NC), iz).reshape(CX + 2, ROWS, 2 * BZ)

    def put(ref, X, h, four):
        for a in range(4):
            ref[X, h, pl.ds(a, CY, stride=4), :] = four[a]

    for X in (0, CX + 1):
        for h in range(2):
            put(corr, X, h, [pz[X, 0:CY, 128 * h : 128 * (h + 1)]] * 4)

    def prolong(X, carry):
        row = iota((CY, 128), 0)
        for h in range(2):
            lanes = slice(128 * h, 128 * (h + 1))
            here = pz[X, 0:CY, lanes]
            base = pz[X, 0:CY, BZ + 128 * h : BZ + 128 * (h + 1)]
            below = jnp.where(row == 0, pz[X, CY : CY + 1, lanes], pltpu.roll(here, 1, 0))
            above = jnp.where(row == CY - 1, pz[X, CY + 1 : CY + 2, lanes], pltpu.roll(here, CY - 1, 0))
            put(corr, X, h, [here] * 4)
            put(shift, X - 1, h, [base + (here - below), base, base, base + (here - above)])
        return carry

    def by_two(body):
        return lambda i, carry: body(2 * i + 1, body(2 * i, carry))

    lax.fori_loop(0, CX // 2, by_two(lambda X, carry: prolong(X + 1, carry)), 0)

    def final_residual(X, h):
        here = corr[X + 1, h]
        within = shift[X, h]
        planes = [rs[4 * X + j, h] - within for j in range(4)]
        planes[0] = planes[0] - (here - corr[X, h])
        planes[3] = planes[3] - (here - corr[X + 2, h])
        return here, planes

    def add_squares(X, total):
        for h in range(2):
            _, planes = final_residual(X, h)
            for out in planes:
                total = total + (out * out).reshape(8, 8, 128).sum(axis=0)
        return total

    def finish(X, carry):
        for h in range(2):
            here, planes = final_residual(X, h)
            lanes = slice(128 * h, 128 * (h + 1))
            for j in range(4):
                up_ref[4 * X + j, :, lanes] = w[4 * X + j + 1, h, MID, :] + here
                new_ref[4 * X + j, :, lanes] = planes[j]
        return carry

    total = lax.fori_loop(0, CX // 2, by_two(add_squares), jnp.zeros((8, 128), F32))

    one = pl.ds(0, 1)
    n_send[...] = jnp.broadcast_to(jnp.sum(total, axis=0, keepdims=True), (8, 128))

    def copy_n(t, slot):
        return remote(n_send.at[one], n_recv.at[slot, one], n_ss.at[t], n_rs.at[slot], of_group(t))

    others(lambda t: copy_n(t, me).start())
    lax.fori_loop(0, CX // 2, by_two(finish), 0)
    n_recv[me, 0:1, :] = n_send[0:1, :]
    others(lambda t: copy_n(t, t).wait_recv())
    total = n_recv[0, 0:1, :]
    for t in range(1, GROUP):
        total = total + n_recv[t, 0:1, :]
    n_held[0:1, :] = total

    def copy_l(d):
        to, slot = lax.rem(bx + d, GX), lax.rem(bx + GX - d, GX)
        return (
            remote(n_held.at[one], n_last.at[bx, one], l_ss.at[d], l_rs.at[bx], {"gx": to}),
            remote(n_held.at[one], n_last.at[slot, one], l_ss.at[d], l_rs.at[slot], {"gx": to}),
        )

    line = [copy_l(d) for d in range(1, GX)]
    for out, _ in line:
        out.start()
    n_last[bx, 0:1, :] = total
    for _, back in line:
        back.wait_recv()
    total = n_last[0, 0:1, :]
    for b in range(1, GX):
        total = total + n_last[b, 0:1, :]
    norm_ref[...] = jnp.sqrt(jnp.full((8, 128), jnp.sum(total), F32))

    for copy in list(g_planes.values()) + list(res_planes.values()) + list(w_planes.values()):
        copy.wait_send()
    for copies in g_rows + res_rows + w_rows + [g_edges, res_edges, w_edges, m_copies, v_copies]:
        for copy in copies:
            copy.wait_send()

    def all_sent(t):
        wait_send(copy_a(t, t))
        wait_send(copy_c(t, t))
        copy_n(t, t).wait_send()

    others(all_sent)
    for out, _ in line:
        out.wait_send()


def hand_on(up, new, norm, up_hbm, new_hbm, norm_out, sems):
    part = BX // 2
    copies = [
        pltpu.make_async_copy(src.at[pl.ds(part * k, part)], dst.at[pl.ds(part * k, part)], sems.at[i, k])
        for k in range(2)
        for i, (src, dst) in enumerate(((up, up_hbm), (new, new_hbm)))
    ]
    for copy in copies:
        copy.start()
    norm_out[0, 0] = norm[0, 0]
    for copy in copies:
        copy.wait()


ANY = pl.BlockSpec(memory_space=pl.ANY)
IN_VMEM = pl.BlockSpec(memory_space=pltpu.VMEM)
DMA = pltpu.SemaphoreType.DMA
VMEM = pltpu.VMEM


def per_device(right_side, guess):
    shape = jax.ShapeDtypeStruct
    block = (BX, BY, BZ)
    padded = (BX + 2, 2, PADDED, 128)
    updated, new_residual, norm = pl.pallas_call(
        kernel,
        out_shape=(shape(block, F32), shape(block, F32), shape((8, 128), F32)),
        in_specs=[ANY] * 2,
        out_specs=(IN_VMEM,) * 3,
        scratch_shapes=[
            VMEM(padded, F32), VMEM((BX, 2, BY, 128), F32), VMEM(padded, F32), VMEM(padded, F32),
            VMEM((2, 2 * BZ, NC), BF16), VMEM((2, NC, 2 * BZ), BF16), VMEM((2, NC, NC), BF16),
            VMEM((2, NC, GY * EXTRA), BF16), VMEM((2, GY * EXTRA, NC), BF16),
            VMEM((4, BY, 128), F32), VMEM((CX, CY, 2 * BZ), F32), VMEM((2, 4 * CX, 128), F32),
            VMEM((CX, CY, 128), F32), VMEM((GROUP, CY, 128), F32), VMEM((GROUP, CY, 128), F32),
            VMEM((GROUP, EXTRA, 128), F32), VMEM((GROUP, EXTRA, 128), F32), VMEM((GY * EXTRA, 128), F32),
            VMEM((CX, 128), F32), VMEM((GX, CX, 128), F32), VMEM((CX, 128), F32), VMEM((2, CX, 128), F32),
            VMEM((GY, CY, 128), F32), VMEM((GROUP, CY, 128), F32),
            VMEM((GY, EXTRA, 128), F32), VMEM((GROUP, EXTRA, 128), F32),
            VMEM((3, PARTS, 16, 128), F32), VMEM((3, PARTS, 16, 128), F32),
            VMEM((CX + 2, ROWS, 128), F32), VMEM((CX + 2, ROWS, 2 * BZ), F32),
            VMEM((CX + 2, 2, BY, 128), F32), VMEM((CX, 2, BY, 128), F32),
            VMEM((8, 128), F32), VMEM((GROUP, 8, 128), F32), VMEM((8, 128), F32), VMEM((GX, 8, 128), F32),
            DMA((LOADS, 2)), DMA((LOADS, 2)), DMA((2,)), DMA((2,)),
            DMA((3, 2)), DMA((3, 2)), DMA((3, PARTS, 2)), DMA((3, PARTS, 2)),
            DMA((3, PARTS)), DMA((3, PARTS)), DMA((GROUP,)), DMA((GROUP,)), DMA((GX,)), DMA((GX,)),
            DMA((GROUP,)), DMA((GROUP,)), DMA((GROUP,)), DMA((GROUP,)), DMA((GROUP,)), DMA((GROUP,)),
            DMA((GROUP,)), DMA((GROUP,)), DMA((GX,)), DMA((GX,)),
        ],
        compiler_params=pltpu.CompilerParams(
            collective_id=0, has_side_effects=True, vmem_limit_bytes=44 * 1024 * 1024
        ),
        name="schwarz",
    )(right_side, guess)
    updated, new_residual, norm = pl.pallas_call(
        hand_on,
        out_shape=(shape(block, F32), shape(block, F32), shape((1, 1), F32)),
        in_specs=[ANY, ANY, IN_VMEM],
        out_specs=(ANY, ANY, pl.BlockSpec(memory_space=pltpu.SMEM)),
        scratch_shapes=[DMA((2, 2))],
        compiler_params=pltpu.CompilerParams(vmem_limit_bytes=1024 * 1024),
        name="hand_on",
    )(updated, new_residual, norm)
    return updated, new_residual, norm.reshape(())


def solution(mesh):
    spec = P("gx", "gy", "gz")
    return jax.shard_map(
        per_device, mesh=mesh, in_specs=(spec, spec), out_specs=(spec, spec, P()), check_vma=False
    )
```
